64 devices in a mesh: dp: 4 (over x, y), cp: 16 (over z, core).
Axes of the slice: x: 2, y: 2, z: 8, core: 2. Of those that a mesh axis runs over, the one named last changes fastest.
The devices are a block of a 4x4x8 slice.
Arguments:
- hidden: bfloat16 [64, 1024, 1152], P('dp', 'cp'), parts along dimension 0
- positions: int32 [64, 1024], P('dp', 'cp'), parts along dimension 0
- wq_local: bfloat16 [1152, 1024], replicated
- wk_local: bfloat16 [1152, 256], replicated
- wv_local: bfloat16 [1152, 256], replicated
- wo_local: bfloat16 [1024, 1152], replicated
- wgate_local: bfloat16 [1152, 6912], replicated
- wup_local: bfloat16 [1152, 6912], replicated
- wdown_local: bfloat16 [6912, 1152], replicated
- preatt_local: float32 [1152], replicated
- postatt_local: float32 [1152], replicated
- preffw_local: float32 [1152], replicated
- postffw_local: float32 [1152], replicated
- wq_global: bfloat16 [1152, 1024], replicated
- wk_global: bfloat16 [1152, 256], replicated
- wv_global: bfloat16 [1152, 256], replicated
- wo_global: bfloat16 [1024, 1152], replicated
- wgate_global: bfloat16 [1152, 6912], replicated
- wup_global: bfloat16 [1152, 6912], replicated
- wdown_global: bfloat16 [6912, 1152], replicated
- preatt_global: float32 [1152], replicated
- postatt_global: float32 [1152], replicated
- preffw_global: float32 [1152], replicated
- postffw_global: float32 [1152], replicated
Outputs:
- output: bfloat16 [64, 1024, 1152], P('dp', 'cp'), parts along dimension 0
There are 4 independent parts. The reference program is written for one: setup_inputs(seed, part) draws one part's arguments, and reference() takes and returns one part's arrays. A program takes and returns all parts, laid end to end along the dimension named above; an argument that names none is the same for every part.
All inputs are finite; a program needn't handle non-finite values.
Results may differ from the reference program's by a relative error of at most 0.02.
Values are sent between devices in bfloat16 or wider.
A program may use at most 768 MiB of HBM per device.

```python
import jax
import jax.numpy as jnp
from jax import lax

BATCH_ROWS = 16
SEQ_LEN = 1024
BLOCK_LEN = 64
MODEL_DIM = 1152
NUM_HEADS = 4
KV_HEADS = 1
HEAD_DIM = 256
FFN_DIM = 6912
WINDOW = 512
NUM_BLOCKS = SEQ_LEN // BLOCK_LEN
GROUP_SIZE = NUM_HEADS // KV_HEADS
EPSILON = 1e-6
THETA = 10000.0
SOFT_CAP = 50.0
LAYER_TAGS = ("local", "global")
WEIGHT_NAMES = ("wq", "wk", "wv", "wo", "wgate", "wup", "wdown")
SCALE_NAMES = ("preatt", "postatt", "preffw", "postffw")


def layer_weights(rng_key, layer_tag):
    key_list = jax.random.split(rng_key, 11)
    q_width = NUM_HEADS * HEAD_DIM
    kv_width = KV_HEADS * HEAD_DIM
    shapes = ((MODEL_DIM, q_width), (MODEL_DIM, kv_width), (MODEL_DIM, kv_width), (q_width, MODEL_DIM), (MODEL_DIM, FFN_DIM), (MODEL_DIM, FFN_DIM), (FFN_DIM, MODEL_DIM))
    weights = {}
    for slot_idx in range(7):
        fan_in, fan_out = shapes[slot_idx]
        drawn = jax.random.normal(key_list[slot_idx], (fan_in, fan_out), jnp.float32) * fan_in ** -0.5
        weights[WEIGHT_NAMES[slot_idx] + "_" + layer_tag] = drawn.astype(jnp.bfloat16)
    for slot_idx in range(4):
        weights[SCALE_NAMES[slot_idx] + "_" + layer_tag] = 0.4 * jax.random.normal(key_list[7 + slot_idx], (MODEL_DIM,), jnp.float32)
    return weights


def setup_inputs(seed: int = 0, part: int = 0) -> dict:
    part_key = jax.random.fold_in(jax.random.key(seed), part)
    key_hidden, key_steps = jax.random.split(part_key)
    hidden = jax.random.normal(key_hidden, (BATCH_ROWS, SEQ_LEN, MODEL_DIM), jnp.float32).astype(jnp.bfloat16)
    step_sizes = jax.random.randint(key_steps, (BATCH_ROWS, SEQ_LEN), 1, 3, jnp.int32)
    positions = (jnp.cumsum(step_sizes, axis=1) - step_sizes[:, :1]).astype(jnp.int32)
    inputs = {"hidden": hidden, "positions": positions}
    weight_key = jax.random.key(seed + 1)
    for layer_idx in range(2):
        inputs.update(layer_weights(jax.random.fold_in(weight_key, layer_idx), LAYER_TAGS[layer_idx]))
    return inputs


def rms_norm(inputs, norm_scale):
    widened = inputs.astype(jnp.float32)
    mean_sq = jnp.mean(widened * widened, axis=-1, keepdims=True)
    return (widened * lax.rsqrt(mean_sq + EPSILON) * (1.0 + norm_scale)).astype(jnp.bfloat16)


def mat_mul(inputs, weight):
    flat_in = inputs.reshape(-1, inputs.shape[-1])
    product = jnp.dot(flat_in, weight, preferred_element_type=jnp.float32)
    return product.reshape(inputs.shape[:-1] + (weight.shape[1],)).astype(jnp.bfloat16)


def apply_rope(heads_in, positions):
    half_dim = HEAD_DIM // 2
    inv_freq = THETA ** (-(jnp.arange(half_dim, dtype=jnp.float32) * 2.0 / HEAD_DIM))
    angles = positions.astype(jnp.float32)[:, :, None, None] * inv_freq
    cos_t = jnp.cos(angles)
    sin_t = jnp.sin(angles)
    widened = heads_in.astype(jnp.float32)
    first_half = widened[..., :half_dim]
    second_half = widened[..., half_dim:]
    return jnp.concatenate([first_half * cos_t - second_half * sin_t, second_half * cos_t + first_half * sin_t], axis=-1)


def decoder_layer(hidden, positions, weights, window_len):
    w_q, w_k, w_v, w_o, w_gate, w_up, w_down, pre_att, post_att, pre_ffw, post_ffw = weights
    normed = rms_norm(hidden, pre_att)
    query_rot = apply_rope(mat_mul(normed, w_q).reshape(BATCH_ROWS, SEQ_LEN, NUM_HEADS, HEAD_DIM), positions)
    query_rot = (query_rot * HEAD_DIM ** -0.5).astype(jnp.bfloat16)
    key_rot = apply_rope(mat_mul(normed, w_k).reshape(BATCH_ROWS, SEQ_LEN, KV_HEADS, HEAD_DIM), positions).astype(jnp.bfloat16)
    value_t = mat_mul(normed, w_v).reshape(BATCH_ROWS, SEQ_LEN, KV_HEADS, HEAD_DIM)
    key_wide = key_rot.astype(jnp.float32)
    value_wide = value_t.astype(jnp.float32)
    q_blocks = query_rot.reshape(BATCH_ROWS, NUM_BLOCKS, BLOCK_LEN, KV_HEADS, GROUP_SIZE, HEAD_DIM).transpose(1, 0, 2, 3, 4, 5)
    pos_blocks = positions.reshape(BATCH_ROWS, NUM_BLOCKS, BLOCK_LEN).transpose(1, 0, 2)
    hid_blocks = hidden.reshape(BATCH_ROWS, NUM_BLOCKS, BLOCK_LEN, MODEL_DIM).transpose(1, 0, 2, 3)

    def one_block(block_in):
        q_block, q_pos, h_block = block_in
        scores = jnp.einsum("bqkgd,bskd->bkgqs", q_block.astype(jnp.float32), key_wide)
        capped = SOFT_CAP * jnp.tanh(scores / SOFT_CAP)
        offset = q_pos[:, None, None, :, None] - positions[:, None, None, None, :]
        visible = (offset >= 0) & (offset < window_len)
        prob_bf = jax.nn.softmax(jnp.where(visible, capped, -1e30), axis=-1).astype(jnp.bfloat16)
        mixed_heads = jnp.einsum("bkgqs,bskd->bqkgd", prob_bf.astype(jnp.float32), value_wide).astype(jnp.bfloat16)
        attn_out = mat_mul(mixed_heads.reshape(BATCH_ROWS, BLOCK_LEN, NUM_HEADS * HEAD_DIM), w_o)
        mid_state = (h_block.astype(jnp.float32) + rms_norm(attn_out, post_att).astype(jnp.float32)).astype(jnp.bfloat16)
        normed_mid = rms_norm(mid_state, pre_ffw)
        gate_val = mat_mul(normed_mid, w_gate)
        up_val = mat_mul(normed_mid, w_up)
        act_val = (jax.nn.gelu(gate_val.astype(jnp.float32), approximate=True) * up_val.astype(jnp.float32)).astype(jnp.bfloat16)
        down_val = mat_mul(act_val, w_down)
        return (mid_state.astype(jnp.float32) + rms_norm(down_val, post_ffw).astype(jnp.float32)).astype(jnp.bfloat16)

    out_blocks = lax.map(one_block, (q_blocks, pos_blocks, hid_blocks))
    return out_blocks.transpose(1, 0, 2, 3).reshape(BATCH_ROWS, SEQ_LEN, MODEL_DIM)


def reference(hidden, positions, wq_local, wk_local, wv_local, wo_local, wgate_local, wup_local, wdown_local, preatt_local, postatt_local, preffw_local, postffw_local, wq_global, wk_global, wv_global, wo_global, wgate_global, wup_global, wdown_global, preatt_global, postatt_global, preffw_global, postffw_global):
    local_set = (wq_local, wk_local, wv_local, wo_local, wgate_local, wup_local, wdown_local, preatt_local, postatt_local, preffw_local, postffw_local)
    global_set = (wq_global, wk_global, wv_global, wo_global, wgate_global, wup_global, wdown_global, preatt_global, postatt_global, preffw_global, postffw_global)
    mid_hidden = decoder_layer(hidden, positions, local_set, WINDOW)
    return decoder_layer(mid_hidden, positions, global_set, 2 * SEQ_LEN)
```

```python
import functools

import jax
import jax.numpy as jnp
from jax import lax
from jax.experimental import pallas as pl
from jax.experimental.pallas import tpu as pltpu
from jax.sharding import PartitionSpec as P

HEAD_DIM = 256
HALF_DIM = HEAD_DIM // 2
WINDOW = 512
EPSILON = 1e-6
THETA = 10000.0
SOFT_CAP = 50.0
LOG2E = 1.4426950408889634
GELU_A = 0.7978845608028654
F_TILE = 768
RING = 4
BF16 = jnp.bfloat16
F32 = jnp.float32


def dot(lhs, rhs):
    return jnp.dot(lhs, rhs, preferred_element_type=F32)


def gelu_times(gate, up):
    gate = gate.astype(BF16).astype(F32)
    up = up.astype(BF16).astype(F32)
    inner = gate * (GELU_A + (GELU_A * 0.044715) * (gate * gate))
    scaled = (0.5 * gate) * up
    return (scaled + scaled * jnp.tanh(inner)).astype(BF16)


def rms(rows, scale):
    mean_sq = jnp.mean(rows * rows, axis=-1, keepdims=True)
    return (rows * lax.rsqrt(mean_sq + EPSILON) * scale).astype(BF16)


def rope(raw, cos_t, sin_t):
    raw = raw.astype(BF16).astype(F32)
    first, second = raw[:, :HALF_DIM], raw[:, HALF_DIM:]
    return first * cos_t - second * sin_t, second * cos_t + first * sin_t


def fused_kernel(cp_size, hidden, pos_rows, scales, inv_freq, *refs):
    weights = (refs[0:7], refs[7:14])
    out = refs[14]
    (xb, ab, qs, kb, vb, ob, oacc, lacc, posb, pcol, prow, cos_b, sin_b, acc, hb, w_qkv, w_o, w_g, w_u, w_d,
     w_sem, ring_sem, x_send, x_recv, p_send, p_recv, kv_send, kv_recv, o_send, o_recv) = refs[15:]
    n_chips = cp_size // 2
    piece = hidden.shape[1]
    dim = hidden.shape[2]
    slots = xb.shape[1] // piece
    quarter = slots // 2
    q_len = quarter * piece
    n_tok = xb.shape[1]
    n_heads = w_o.shape[1] // HEAD_DIM
    ffn = weights[0][4].shape[1]
    n_tiles = ffn // F_TILE
    me = lax.axis_index("cp")
    chip, core = me // 2, me % 2
    my_quarter = me // quarter
    my_core = jnp.where((my_quarter == 0) | (my_quarter == 3), 0, 1)
    my_slot = me % quarter + jnp.where(my_quarter >= 2, quarter, 0)

    def quarter_of(which_core, idx):
        return which_core + idx * (3 - 2 * which_core)

    w_copies = []
    for layer in range(2):
        wq, wk, wv, wo = weights[layer][:4]
        q_wide = wq.shape[1]
        w_copies += [
            pltpu.make_async_copy(wq, w_qkv.at[layer, :, pl.ds(0, q_wide)], w_sem.at[layer, 0]),
            pltpu.make_async_copy(wk, w_qkv.at[layer, :, pl.ds(q_wide, HEAD_DIM)], w_sem.at[layer, 1]),
            pltpu.make_async_copy(wv, w_qkv.at[layer, :, pl.ds(q_wide + HEAD_DIM, HEAD_DIM)], w_sem.at[layer, 2]),
            pltpu.make_async_copy(wo, w_o.at[layer], w_sem.at[layer, 3]),
        ]

    def tile_copies(layer, tile, buf):
        gate, up, down = weights[layer][4:7]
        cols = pl.ds(pl.multiple_of(tile * F_TILE, F_TILE), F_TILE)
        return (
            pltpu.make_async_copy(gate.at[:, cols], w_g.at[buf], ring_sem.at[0, buf]),
            pltpu.make_async_copy(up.at[:, cols], w_u.at[buf], ring_sem.at[1, buf]),
            pltpu.make_async_copy(down.at[cols, :], w_d.at[buf], ring_sem.at[2, buf]),
        )

    def start_tile(count):
        layer, tile, buf = (count // n_tiles) % 2, count % n_tiles, count % RING

        @pl.when(layer == 0)
        def _():
            for copy in tile_copies(0, tile, buf):
                copy.start()

        @pl.when(layer == 1)
        def _():
            for copy in tile_copies(1, tile, buf):
                copy.start()

    barrier = pltpu.get_barrier_semaphore()
    for shift in range(1, cp_size):
        pl.semaphore_signal(barrier, inc=1, device_id={"cp": lax.rem(me + shift, cp_size)}, device_id_type=pl.DeviceIdType.MESH)
    pl.semaphore_wait(barrier, cp_size - 1)

    order = sorted(range(1, n_chips), key=lambda d: -min(d, n_chips - d)) + [0]

    def x_copy(half, shift):
        to_chip = lax.rem(chip + shift, n_chips)
        return pltpu.make_async_remote_copy(
            src_ref=hidden.at[half * n_chips + to_chip], dst_ref=xb.at[half, pl.ds(my_slot * piece, piece), :],
            send_sem=x_send.at[half, shift], recv_sem=x_recv.at[half, my_slot],
            device_id={"cp": 2 * to_chip + my_core}, device_id_type=pl.DeviceIdType.MESH)

    def x_local(half):
        return pltpu.make_async_copy(hidden.at[half * n_chips + chip], xb.at[half, pl.ds(my_slot * piece, piece), :], x_recv.at[half, my_slot])

    def p_copy(shift, to_core):
        to_chip = lax.rem(chip + shift, n_chips)
        return pltpu.make_async_remote_copy(
            src_ref=pos_rows.at[to_chip], dst_ref=posb.at[me], send_sem=p_send.at[shift, to_core], recv_sem=p_recv.at[me],
            device_id={"cp": 2 * to_chip + to_core}, device_id_type=pl.DeviceIdType.MESH)

    def p_local():
        return pltpu.make_async_copy(pos_rows.at[chip], posb.at[me], p_recv.at[me])

    for shift in order:
        for to_core in range(2):
            if shift:
                p_copy(shift, to_core).start()
            else:
                @pl.when(core != to_core)
                def _():
                    p_copy(shift, to_core).start()
    p_local().start()
    for half in range(2):
        for shift in order:
            if shift:
                x_copy(half, shift).start()
            else:
                @pl.when(my_core != core)
                def _():
                    x_copy(half, shift).start()

                @pl.when(my_core == core)
                def _():
                    x_local(half).start()

    for copy in w_copies:
        copy.start()
    for count in range(RING - 1):
        start_tile(count)

    for from_piece in range(cp_size):
        pltpu.make_async_copy(pos_rows.at[0], posb.at[from_piece], p_recv.at[from_piece]).wait()
    for copy in w_copies:
        copy.wait()

    def kv_copy(slot, idx, which):
        buf = (kb, vb)[which]
        rows = pl.ds(pl.multiple_of(quarter_of(core, idx) * q_len, q_len), q_len)
        return pltpu.make_async_remote_copy(
            src_ref=buf.at[slot, rows, :], dst_ref=buf.at[slot, rows, :], send_sem=kv_send.at[slot, idx, which],
            recv_sem=kv_recv.at[slot, idx, which], device_id={"cp": 2 * chip + 1 - core}, device_id_type=pl.DeviceIdType.MESH)

    def o_copy(half, slot):
        idx = slot // quarter
        to_piece = quarter_of(core, idx) * quarter + slot % quarter
        return to_piece, pltpu.make_async_remote_copy(
            src_ref=xb.at[half, pl.ds(slot * piece, piece), :], dst_ref=out.at[half * n_chips + chip],
            send_sem=o_send.at[half, slot], recv_sem=o_recv.at[half, chip],
            device_id={"cp": to_piece}, device_id_type=pl.DeviceIdType.MESH)

    def stage(count, carry):
        half, layer = count // 2, count % 2
        kv_slot = count % 2

        @pl.when(layer == 0)
        def _():
            for slot in range(slots):
                pltpu.make_async_copy(hidden.at[0], xb.at[half, pl.ds(slot * piece, piece), :], x_recv.at[half, slot]).wait()
            lane = lax.broadcasted_iota(jnp.int32, (1, 2 * piece), 1)
            for quad in range(4):
                for pair in range(quarter // 2):
                    even = posb[quad * quarter + 2 * pair, pl.ds(half, 1), :]
                    odd = posb[quad * quarter + 2 * pair + 1, pl.ds(half, 1), :]
                    prow[quad, :, pl.ds(pair * 2 * piece, 2 * piece)] = jnp.broadcast_to(jnp.where(lane < piece, even, odd), (8, 2 * piece))
            for idx in range(2):
                for pair in range(quarter // 2):
                    line = prow[quarter_of(core, idx), pl.ds(0, 1), pl.ds(pair * 2 * piece, 2 * piece)]
                    column = jnp.broadcast_to(line, (2 * piece, 2 * piece)).T
                    rows = pl.ds(idx * q_len + pair * 2 * piece, 2 * piece)
                    pcol[rows, :] = column
                    angle = column * inv_freq[...]
                    cos_b[rows, :] = jnp.cos(angle)
                    sin_b[rows, :] = jnp.sin(angle)

        def norm_in(step, inner):
            rows = pl.ds(pl.multiple_of(step * 32, 32), 32)
            ab[rows, :] = rms(xb[half, rows, :].astype(F32), scales[layer, pl.ds(0, 1), :])
            return inner

        lax.fori_loop(0, n_tok // 32, norm_in, 0)

        q_wide = n_heads * HEAD_DIM
        for idx in range(2):
            rows = pl.ds(idx * q_len, q_len)
            home = pl.ds(pl.multiple_of(quarter_of(core, idx) * q_len, q_len), q_len)
            kv = dot(ab[rows, :], w_qkv[layer, :, q_wide:])
            low, high = rope(kv[:, :HEAD_DIM], cos_b[rows, :], sin_b[rows, :])
            kb[kv_slot, home, pl.ds(0, HALF_DIM)] = low.astype(BF16)
            kb[kv_slot, home, pl.ds(HALF_DIM, HALF_DIM)] = high.astype(BF16)
            vb[kv_slot, home, :] = kv[:, HEAD_DIM:].astype(BF16)
        for idx in range(2):
            for which in range(2):
                kv_copy(kv_slot, idx, which).start()
        for idx in range(2):
            rows = pl.ds(idx * q_len, q_len)
            for head in range(n_heads):
                raw = dot(ab[rows, :], w_qkv[layer, :, pl.ds(head * HEAD_DIM, HEAD_DIM)])
                low, high = rope(raw, cos_b[rows, :], sin_b[rows, :])
                there = pl.ds(head * q_len, q_len)
                qs[idx, there, pl.ds(0, HALF_DIM)] = (low * HEAD_DIM ** -0.5).astype(BF16)
                qs[idx, there, pl.ds(HALF_DIM, HALF_DIM)] = (high * HEAD_DIM ** -0.5).astype(BF16)
        for idx in range(2):
            for which in range(2):
                theirs = pl.ds(pl.multiple_of(quarter_of(1 - core, idx) * q_len, q_len), q_len)
                buf = (kb, vb)[which]
                pltpu.make_async_remote_copy(
                    src_ref=buf.at[kv_slot, theirs, :], dst_ref=buf.at[kv_slot, theirs, :], send_sem=kv_send.at[kv_slot, idx, which],
                    recv_sem=kv_recv.at[kv_slot, idx, which], device_id={"cp": 2 * chip + 1 - core}, device_id_type=pl.DeviceIdType.MESH).wait_recv()

        centre = jnp.where(layer == 0, (WINDOW - 1) * 0.5, n_tok * 2.0 - 0.5)
        for idx in range(2):
            quad = quarter_of(core, idx)
            lowest = jnp.where(layer == 0, jnp.maximum(quad - WINDOW // q_len, 0), 0)
            oacc[...] = jnp.zeros_like(oacc)
            lacc[...] = jnp.zeros_like(lacc)

            def key_block(block, inner):
                keys = pl.ds(pl.multiple_of(block * q_len, q_len), q_len)
                k_tile = kb[kv_slot, keys, :]
                v_tile = vb[kv_slot, keys, :]
                here = pcol[pl.ds(idx * q_len, q_len), :] - centre
                there = prow[block, pl.ds(0, 1), :]
                seen = jnp.concatenate([jnp.abs(here - there[:, :HALF_DIM]) <= centre, jnp.abs(here - there[:, HALF_DIM:]) <= centre], axis=1)
                for head in range(n_heads):
                    rows = pl.ds(head * q_len, q_len)
                    scores = lax.dot_general(qs[idx, rows, :], k_tile, (((1,), (1,)), ((), ())), preferred_element_type=F32)
                    expd = jnp.where(seen, jnp.exp2((SOFT_CAP * LOG2E) * jnp.tanh(scores * (1.0 / SOFT_CAP))), 0.0)
                    lacc[rows, :] += expd[:, :HALF_DIM] + expd[:, HALF_DIM:]
                    oacc[rows, :] += dot(expd.astype(BF16), v_tile)
                return inner

            lax.fori_loop(lowest, quad + 1, key_block, 0)
            for head in range(n_heads):
                rows = pl.ds(head * q_len, q_len)
                total = jnp.sum(lacc[rows, :], axis=1, keepdims=True)
                ob[pl.ds(idx * q_len, q_len), pl.ds(head * HEAD_DIM, HEAD_DIM)] = (oacc[rows, :] / total).astype(BF16)

        acc[...] = dot(ob[...], w_o[layer])

        def norm_mid(step, inner):
            rows = pl.ds(pl.multiple_of(step * 16, 16), 16)
            attn = acc[rows, :].astype(BF16).astype(F32)
            mid = (xb[half, rows, :].astype(F32) + rms(attn, scales[layer, pl.ds(1, 1), :]).astype(F32)).astype(BF16)
            xb[half, rows, :] = mid
            ab[rows, :] = rms(mid.astype(F32), scales[layer, pl.ds(2, 1), :])
            acc[rows, :] = jnp.zeros((16, dim), F32)
            return inner

        lax.fori_loop(0, n_tok // 16, norm_mid, 0)

        def ffn_tile(tile, inner):
            now = count * n_tiles + tile
            buf = now % RING
            for copy in tile_copies(0, 0, buf):
                copy.wait()

            @pl.when(now + RING - 1 < 4 * n_tiles)
            def _():
                start_tile(now + RING - 1)

            hb[...] = gelu_times(dot(ab[...], w_g[buf]), dot(ab[...], w_u[buf]))
            acc[...] += dot(hb[...], w_d[buf])
            return inner

        lax.fori_loop(0, n_tiles, ffn_tile, 0)

        def norm_out(step, inner):
            rows = pl.ds(pl.multiple_of(step * 16, 16), 16)
            down = acc[rows, :].astype(BF16).astype(F32)
            xb[half, rows, :] = (xb[half, rows, :].astype(F32) + rms(down, scales[layer, pl.ds(3, 1), :]).astype(F32)).astype(BF16)
            return inner

        lax.fori_loop(0, n_tok // 16, norm_out, 0)
        for idx in range(2):
            for which in range(2):
                kv_copy(kv_slot, idx, which).wait_send()

        @pl.when(layer == 1)
        def _():
            for slot in range(slots):
                to_piece, copy = o_copy(half, slot)

                @pl.when(to_piece != me)
                def _():
                    copy.start()

                @pl.when(to_piece == me)
                def _():
                    pltpu.make_async_copy(xb.at[half, pl.ds(slot * piece, piece), :], out.at[half * n_chips + chip], o_recv.at[half, chip]).start()

        return carry

    lax.fori_loop(0, 4, stage, 0)

    for half in range(2):
        for slot in range(slots):
            to_piece, copy = o_copy(half, slot)

            @pl.when(to_piece != me)
            def _():
                copy.wait_send()
        for from_chip in range(n_chips):
            pltpu.make_async_copy(xb.at[half, pl.ds(0, piece), :], out.at[half * n_chips + from_chip], o_recv.at[half, from_chip]).wait()
        for shift in order:
            if shift:
                x_copy(half, shift).wait_send()
            else:
                @pl.when(my_core != core)
                def _():
                    x_copy(half, shift).wait_send()
    for shift in order:
        for to_core in range(2):
            if shift:
                p_copy(shift, to_core).wait_send()
            else:
                @pl.when(core != to_core)
                def _():
                    p_copy(shift, to_core).wait_send()


def solution(mesh):
    cp_size = mesh.shape["cp"]

    def device_step(hidden, positions, *weights):
        rows, piece, dim = hidden.shape
        n_chips = cp_size // 2
        n_tok = piece * cp_size // 2
        q_wide = weights[0].shape[1]
        ffn = weights[4].shape[1]
        n_heads = q_wide // HEAD_DIM
        q_len = n_tok // 2
        pos = positions.astype(F32).reshape(2, n_chips, piece).transpose(1, 0, 2)
        pos = jnp.pad(jnp.concatenate([pos, pos], axis=2), ((0, 0), (0, 6), (0, 0)))
        scales = 1.0 + jnp.stack([jnp.stack(weights[7:11]), jnp.stack(weights[18:22])])
        inv_freq = (THETA ** (-(jnp.arange(HALF_DIM, dtype=F32) * 2.0 / HEAD_DIM)))[None, :]
        matrices = weights[0:7] + weights[11:18]
        hbm = pl.BlockSpec(memory_space=pltpu.HBM)
        vmem = pl.BlockSpec(memory_space=pltpu.VMEM)
        scratch = [
            pltpu.VMEM((2, n_tok, dim), BF16),
            pltpu.VMEM((n_tok, dim), BF16),
            pltpu.VMEM((2, n_heads * q_len, HEAD_DIM), BF16),
            pltpu.VMEM((2, 2 * n_tok, HEAD_DIM), BF16),
            pltpu.VMEM((2, 2 * n_tok, HEAD_DIM), BF16),
            pltpu.VMEM((n_tok, q_wide), BF16),
            pltpu.VMEM((n_heads * q_len, HEAD_DIM), F32),
            pltpu.VMEM((n_heads * q_len, HALF_DIM), F32),
            pltpu.VMEM((cp_size, 8, 2 * piece), F32),
            pltpu.VMEM((n_tok, HALF_DIM), F32),
            pltpu.VMEM((4, 8, q_len), F32),
            pltpu.VMEM((n_tok, HALF_DIM), F32),
            pltpu.VMEM((n_tok, HALF_DIM), F32),
            pltpu.VMEM((n_tok, dim), F32),
            pltpu.VMEM((n_tok, F_TILE), BF16),
            pltpu.VMEM((2, dim, q_wide + 2 * HEAD_DIM), BF16),
            pltpu.VMEM((2, q_wide, dim), BF16),
            pltpu.VMEM((RING, dim, F_TILE), BF16),
            pltpu.VMEM((RING, dim, F_TILE), BF16),
            pltpu.VMEM((RING, F_TILE, dim), BF16),
            pltpu.SemaphoreType.DMA((2, 4)),
            pltpu.SemaphoreType.DMA((3, RING)),
            pltpu.SemaphoreType.DMA((2, n_chips)),
            pltpu.SemaphoreType.DMA((2, n_chips)),
            pltpu.SemaphoreType.DMA((n_chips, 2)),
            pltpu.SemaphoreType.DMA((cp_size,)),
            pltpu.SemaphoreType.DMA((2, 2, 2)),
            pltpu.SemaphoreType.DMA((2, 2, 2)),
            pltpu.SemaphoreType.DMA((2, n_chips)),
            pltpu.SemaphoreType.DMA((2, n_chips)),
        ]
        return pl.pallas_call(
            functools.partial(fused_kernel, cp_size),
            out_shape=jax.ShapeDtypeStruct(hidden.shape, BF16),
            in_specs=[hbm, hbm, vmem, vmem] + [hbm] * 14,
            out_specs=hbm,
            scratch_shapes=scratch,
            compiler_params=pltpu.CompilerParams(collective_id=0, has_side_effects=True, vmem_limit_bytes=62 * 2 ** 20),
            name="two_layers",
        )(hidden, pos, scales, inv_freq, *matrices)

    specs_in = tuple([P("dp", "cp"), P("dp", "cp")] + [P()] * 22)
    return jax.shard_map(device_step, mesh=mesh, in_specs=specs_in, out_specs=P("dp", "cp"), check_vma=False)
```

```python
import functools

import jax
import jax.numpy as jnp
import numpy as np
from jax import lax
from jax.experimental import pallas as pl
from jax.experimental.pallas import tpu as pltpu
from jax.sharding import PartitionSpec as P

HEAD_DIM = 256
HALF_DIM = HEAD_DIM // 2
WINDOW = 512
EPSILON = 1e-6
THETA = 10000.0
SOFT_CAP = 50.0
LOG2E = 1.4426950408889634
GELU_A = 0.7978845608028654
F_TILE = 2304
F_SUB = 768
BF16 = jnp.bfloat16
F32 = jnp.float32


def dot(lhs, rhs):
    return jnp.dot(lhs, rhs, preferred_element_type=F32)


def gelu_times(gate, up):
    gate = gate.astype(BF16).astype(F32)
    up = up.astype(BF16).astype(F32)
    inner = gate * (GELU_A + (GELU_A * 0.044715) * (gate * gate))
    scaled = (0.5 * gate) * up
    return (scaled + scaled * jnp.tanh(inner)).astype(BF16)


def rms(rows, scale):
    mean_sq = jnp.mean(rows * rows, axis=-1, keepdims=True)
    return (rows * lax.rsqrt(mean_sq + EPSILON) * scale).astype(BF16)


def rope(raw, cos_t, sin_t):
    raw = raw.astype(BF16).astype(F32)
    first, second = raw[:, :HALF_DIM], raw[:, HALF_DIM:]
    return first * cos_t - second * sin_t, second * cos_t + first * sin_t


def fused_kernel(cp_size, hidden, positions, inv_freq, *refs):
    raw_scales = (refs[0:4], refs[4:8])
    weights = (refs[8:15], refs[15:22])
    out = refs[22]
    (xb, ab, qs, kb, vb, ob, mid_b, mask_b, ptile, posb, pcol, prow, cos_b, sin_b, scales, acc, hb, w_qkv, w_o, w_g, w_u, w_d,
     w_sem, ring_sem, x_send, x_recv, p_send, p_recv, kv_send, kv_recv, o_send, o_recv) = refs[23:]
    n_chips = cp_size // 2
    piece = hidden.shape[1]
    dim = hidden.shape[2]
    n_tok = xb.shape[1]
    slots = n_tok // piece
    quarter = slots // 2
    q_len = n_tok // 2
    n_heads = w_o.shape[1] // HEAD_DIM
    q_wide = n_heads * HEAD_DIM
    n_tiles = weights[0][4].shape[1] // F_TILE
    me = lax.axis_index("cp")
    chip, core = me // 2, me % 2
    my_quarter = me // quarter
    my_core = jnp.where((my_quarter == 0) | (my_quarter == 3), 0, 1)
    my_slot = me % quarter + jnp.where(my_quarter >= 2, quarter, 0)

    def quarter_of(which_core, idx):
        return which_core + idx * (3 - 2 * which_core)

    def rows_of(start, size):
        return pl.ds(pl.multiple_of(start, size), size)

    w_copies = []
    for layer in range(2):
        wq, wk, wv, wo = weights[layer][:4]
        w_copies.append((
            pltpu.make_async_copy(wq, w_qkv.at[layer, :, pl.ds(0, q_wide)], w_sem.at[layer, 0]),
            pltpu.make_async_copy(wk, w_qkv.at[layer, :, pl.ds(q_wide, HEAD_DIM)], w_sem.at[layer, 1]),
            pltpu.make_async_copy(wv, w_qkv.at[layer, :, pl.ds(q_wide + HEAD_DIM, HEAD_DIM)], w_sem.at[layer, 2]),
            pltpu.make_async_copy(wo, w_o.at[layer], w_sem.at[layer, 3]),
        ))

    def tile_copies(layer, tile, buf):
        gate, up, down = weights[layer][4:7]
        cols = rows_of(tile * F_TILE, F_TILE)
        return (
            pltpu.make_async_copy(gate.at[:, cols], w_g.at[buf], ring_sem.at[0, buf]),
            pltpu.make_async_copy(up.at[:, cols], w_u.at[buf], ring_sem.at[1, buf]),
            pltpu.make_async_copy(down.at[cols, :], w_d.at[buf], ring_sem.at[2, buf]),
        )

    def start_tile(layer, tile, buf):
        for which in range(2):
            @pl.when(layer == which)
            def _():
                for copy in tile_copies(which, tile, buf):
                    copy.start()

    pos = positions[...].astype(F32)
    pos = jnp.concatenate([pos, pos], axis=1)
    for to_chip in range(n_chips):
        for half in range(2):
            row = half * n_chips + to_chip
            ptile[to_chip, pl.ds(half, 1), :] = pos[row:row + 1, :]
    for layer in range(2):
        for which in range(4):
            scales[layer * 4 + which] = 1.0 + raw_scales[layer][which][...]

    barrier = pltpu.get_barrier_semaphore()
    for shift in range(1, cp_size):
        pl.semaphore_signal(barrier, inc=1, device_id={"cp": lax.rem(me + shift, cp_size)}, device_id_type=pl.DeviceIdType.MESH)
    pl.semaphore_wait(barrier, cp_size - 1)

    def x_copy(half, to_chip):
        return pltpu.make_async_remote_copy(
            src_ref=hidden.at[half * n_chips + to_chip], dst_ref=xb.at[half, rows_of(my_slot * piece, piece), :],
            send_sem=x_send.at[half, to_chip], recv_sem=x_recv.at[half, my_slot],
            device_id={"cp": 2 * to_chip + my_core}, device_id_type=pl.DeviceIdType.MESH)

    def p_copy(to_chip, to_core):
        return pltpu.make_async_remote_copy(
            src_ref=ptile.at[to_chip], dst_ref=posb.at[me], send_sem=p_send.at[to_chip, to_core], recv_sem=p_recv.at[me],
            device_id={"cp": 2 * to_chip + to_core}, device_id_type=pl.DeviceIdType.MESH)

    def each_chip(parity):
        for step in (2, 1, 3, 0):
            yield 2 * lax.rem(chip // 2 + step, n_chips // 2) + parity

    def unless_me(target, copy_call, local_call):
        @pl.when(target != me)
        def _():
            copy_call()

        if local_call is not None:
            @pl.when(target == me)
            def _():
                local_call()

    for parity in range(2):
        for to_chip in each_chip(parity):
            for to_core in range(2):
                unless_me(2 * to_chip + to_core, lambda: p_copy(to_chip, to_core).start(),
                          lambda: pltpu.make_async_copy(ptile.at[to_chip], posb.at[me], p_recv.at[me]).start())
    for half in range(2):
        for parity in range(2):
            for to_chip in each_chip(parity):
                unless_me(2 * to_chip + my_core, lambda: x_copy(half, to_chip).start(),
                          lambda: pltpu.make_async_copy(hidden.at[half * n_chips + to_chip], xb.at[half, rows_of(my_slot * piece, piece), :], x_recv.at[half, my_slot]).start())

    for layer in range(2):
        for copy in w_copies[layer]:
            copy.start()
        start_tile(0, layer, layer)
    for from_piece in range(cp_size):
        pltpu.make_async_copy(ptile.at[0], posb.at[from_piece], p_recv.at[from_piece]).wait()
    for layer in range(2):
        for copy in w_copies[layer]:
            copy.wait()

    def kv_copy(slot, idx, which, owner):
        buf = (kb, vb)[which]
        rows = rows_of(quarter_of(owner, idx) * q_len, q_len)
        return pltpu.make_async_remote_copy(
            src_ref=buf.at[slot, rows, :], dst_ref=buf.at[slot, rows, :], send_sem=kv_send.at[slot, idx, which],
            recv_sem=kv_recv.at[slot, idx, which], device_id={"cp": 2 * chip + 1 - core}, device_id_type=pl.DeviceIdType.MESH)

    def o_target(idx, j):
        return quarter_of(core, idx) * quarter + j

    def o_copy(half, idx, j):
        slot = idx * quarter + j
        return pltpu.make_async_remote_copy(
            src_ref=xb.at[half, rows_of(slot * piece, piece), :], dst_ref=out.at[half * n_chips + chip],
            send_sem=o_send.at[half, slot], recv_sem=o_recv.at[half, chip],
            device_id={"cp": o_target(idx, j)}, device_id_type=pl.DeviceIdType.MESH)

    def stage(count, carry):
        half, layer = count // 2, count % 2
        kv_slot = count % 2

        @pl.when(layer == 0)
        def _():
            for slot in range(slots):
                pltpu.make_async_copy(hidden.at[0], xb.at[half, pl.ds(slot * piece, piece), :], x_recv.at[half, slot]).wait()
            lane = lax.broadcasted_iota(jnp.int32, (1, 2 * piece), 1)
            for quad in range(4):
                for pair in range(quarter // 2):
                    even = posb[quad * quarter + 2 * pair, pl.ds(half, 1), :]
                    odd = posb[quad * quarter + 2 * pair + 1, pl.ds(half, 1), :]
                    prow[quad, :, pl.ds(pair * 2 * piece, 2 * piece)] = jnp.broadcast_to(jnp.where(lane < piece, even, odd), (8, 2 * piece))
            for idx in range(2):
                for pair in range(quarter // 2):
                    line = prow[quarter_of(core, idx), pl.ds(0, 1), pl.ds(pair * 2 * piece, 2 * piece)]
                    column = jnp.broadcast_to(line, (2 * piece, 2 * piece)).T
                    rows = pl.ds(idx * q_len + pair * 2 * piece, 2 * piece)
                    pcol[rows, :] = column
                    angle = column * inv_freq[...]
                    cos_b[rows, :] = jnp.cos(angle)
                    sin_b[rows, :] = jnp.sin(angle)

        pre_att = scales[layer * 4]
        for step in range(n_tok // 16):
            rows = pl.ds(step * 16, 16)
            ab[rows, :] = rms(xb[half, rows, :].astype(F32), pre_att)
        for idx in range(2):
            rows = pl.ds(idx * q_len, q_len)
            home = rows_of(quarter_of(core, idx) * q_len, q_len)
            kv = dot(ab[rows, :], w_qkv[layer, :, q_wide:])
            low, high = rope(kv[:, :HEAD_DIM], cos_b[rows, :], sin_b[rows, :])
            kb[kv_slot, home, pl.ds(0, HALF_DIM)] = low.astype(BF16)
            kb[kv_slot, home, pl.ds(HALF_DIM, HALF_DIM)] = high.astype(BF16)
            vb[kv_slot, home, :] = kv[:, HEAD_DIM:].astype(BF16)
        for idx in range(2):
            for which in range(2):
                kv_copy(kv_slot, idx, which, core).start()
        for idx in range(2):
            rows = pl.ds(idx * q_len, q_len)
            for head in range(n_heads):
                raw = dot(ab[rows, :], w_qkv[layer, :, pl.ds(head * HEAD_DIM, HEAD_DIM)])
                low, high = rope(raw, cos_b[rows, :], sin_b[rows, :])
                there = pl.ds(head * q_len, q_len)
                qs[idx, there, pl.ds(0, HALF_DIM)] = (low * HEAD_DIM ** -0.5).astype(BF16)
                qs[idx, there, pl.ds(HALF_DIM, HALF_DIM)] = (high * HEAD_DIM ** -0.5).astype(BF16)

        pairs = ((0, 0), (1 - core, 1), (1, jnp.where(core == 0, 2, 0)), (1, jnp.where(core == 0, 3, 1)), (1, jnp.where(core == 0, 0, 2)))
        centre = jnp.where(layer == 0, (WINDOW - 1) * 0.5, n_tok * 2.0 - 0.5)
        for number, (idx, block) in enumerate(pairs):
            here = pcol[rows_of(idx * q_len, q_len), :] - centre
            there = prow[block, pl.ds(0, 1), :]
            for part in range(2):
                lanes = pl.ds(part * HALF_DIM, HALF_DIM)
                seen = jnp.abs(here - there[:, part * HALF_DIM:(part + 1) * HALF_DIM]) <= centre
                mask_b[number, :, lanes] = jnp.where(seen, 1.0, 0.0)
        for idx in range(2):
            for which in range(2):
                kv_copy(kv_slot, idx, which, 1 - core).wait_recv()
        to_first = jnp.where(core == 1, 1.0, 0.0)
        to_second = 1.0 - to_first
        for head in range(n_heads):
            sums, values = [], []
            for number, (idx, block) in enumerate(pairs):
                keys = rows_of(block * q_len, q_len)
                scores = lax.dot_general(qs[idx, pl.ds(head * q_len, q_len), :], kb[kv_slot, keys, :], (((1,), (1,)), ((), ())), preferred_element_type=F32)
                expd = jnp.exp2((SOFT_CAP * LOG2E) * jnp.tanh(scores * (1.0 / SOFT_CAP))) * mask_b[number]
                sums.append(expd[:, :HALF_DIM] + expd[:, HALF_DIM:])
                values.append(dot(expd.astype(BF16), vb[kv_slot, keys, :]))
            totals = (sums[0] + to_first * sums[1], (sums[2] + sums[3] + sums[4]) + to_second * sums[1])
            mixed = (values[0] + to_first * values[1], (values[2] + values[3] + values[4]) + to_second * values[1])
            for idx in range(2):
                share = 1.0 / jnp.sum(totals[idx], axis=1, keepdims=True)
                ob[pl.ds(idx * q_len, q_len), pl.ds(head * HEAD_DIM, HEAD_DIM)] = (mixed[idx] * share).astype(BF16)

        post_att, pre_ffw = scales[layer * 4 + 1], scales[layer * 4 + 2]
        for idx in range(2):
            rows = pl.ds(idx * q_len, q_len)
            mid_b[rows, :] = dot(ob[rows, :], w_o[layer])
        for step in range(n_tok // 16):
            rows = pl.ds(step * 16, 16)
            attn = mid_b[rows, :].astype(BF16).astype(F32)
            mid = (xb[half, rows, :].astype(F32) + rms(attn, post_att).astype(F32)).astype(BF16)
            xb[half, rows, :] = mid
            ab[rows, :] = rms(mid.astype(F32), pre_ffw)

        even = count % 2
        post_ffw = scales[layer * 4 + 3]

        def ffn_part(part, inner):
            idx = jnp.where(chip < n_chips // 2, 1 - part, part)
            rows = rows_of(idx * q_len, q_len)
            acc[...] = jnp.zeros_like(acc)

            def ffn_tile(step, inner2):
                buf = (even + step) % 2

                @pl.when((part == 0) | (step == n_tiles - 1))
                def _():
                    for copy in tile_copies(0, 0, buf):
                        copy.wait()

                for sub in range(F_TILE // F_SUB):
                    cols = pl.ds(sub * F_SUB, F_SUB)
                    hb[:, cols] = gelu_times(dot(ab[rows, :], w_g[buf, :, cols]), dot(ab[rows, :], w_u[buf, :, cols]))
                acc[...] += dot(hb[...], w_d[buf])

                @pl.when(step == 0)
                def _():
                    start_tile(layer, (1 - part) * (n_tiles - 1), buf)

                @pl.when((part == 1) & (step > 0) & (count < 3))
                def _():
                    start_tile(1 - layer, step - 1, buf)

                return inner2

            lax.fori_loop(0, n_tiles, ffn_tile, 0)
            for step in range(q_len // 16):
                those = rows_of(idx * q_len + step * 16, 16)
                down = acc[pl.ds(step * 16, 16), :].astype(BF16).astype(F32)
                xb[half, those, :] = (xb[half, those, :].astype(F32) + rms(down, post_ffw).astype(F32)).astype(BF16)

            @pl.when(layer == 1)
            def _():
                for j in range(quarter):
                    unless_me(o_target(idx, j), lambda: o_copy(half, idx, j).start(),
                              lambda: pltpu.make_async_copy(xb.at[half, rows_of((idx * quarter + j) * piece, piece), :], out.at[half * n_chips + chip], o_recv.at[half, chip]).start())

            return inner

        lax.fori_loop(0, 2, ffn_part, 0)
        for idx in range(2):
            for which in range(2):
                kv_copy(kv_slot, idx, which, core).wait_send()
        return carry

    lax.fori_loop(0, 4, stage, 0)

    for half in range(2):
        for idx in range(2):
            for j in range(quarter):
                unless_me(o_target(idx, j), lambda: o_copy(half, idx, j).wait_send(), None)
        for from_chip in range(n_chips):
            pltpu.make_async_copy(xb.at[half, pl.ds(0, piece), :], out.at[half * n_chips + from_chip], o_recv.at[half, from_chip]).wait()
        for to_chip in range(n_chips):
            unless_me(2 * to_chip + my_core, lambda: x_copy(half, to_chip).wait_send(), None)
    for to_chip in range(n_chips):
        for to_core in range(2):
            unless_me(2 * to_chip + to_core, lambda: p_copy(to_chip, to_core).wait_send(), None)


def solution(mesh):
    cp_size = mesh.shape["cp"]

    def device_step(hidden, positions, *weights):
        rows, piece, dim = hidden.shape
        n_chips = cp_size // 2
        n_tok = piece * cp_size // 2
        q_wide = weights[0].shape[1]
        n_heads = q_wide // HEAD_DIM
        q_len = n_tok // 2
        inv_freq = (THETA ** (-(np.arange(HALF_DIM) * 2.0 / HEAD_DIM))).astype(np.float32)[None, :]
        scales = [w[None, :] for w in weights[7:11] + weights[18:22]]
        matrices = weights[0:7] + weights[11:18]
        hbm = pl.BlockSpec(memory_space=pltpu.HBM)
        vmem = pl.BlockSpec(memory_space=pltpu.VMEM)
        scratch = [
            pltpu.VMEM((2, n_tok, dim), BF16),
            pltpu.VMEM((n_tok, dim), BF16),
            pltpu.VMEM((2, n_heads * q_len, HEAD_DIM), BF16),
            pltpu.VMEM((2, 2 * n_tok, HEAD_DIM), BF16),
            pltpu.VMEM((2, 2 * n_tok, HEAD_DIM), BF16),
            pltpu.VMEM((n_tok, q_wide), BF16),
            pltpu.VMEM((n_tok, dim), F32),
            pltpu.VMEM((5, q_len, q_len), F32),
            pltpu.VMEM((n_chips, 8, 2 * piece), F32),
            pltpu.VMEM((cp_size, 8, 2 * piece), F32),
            pltpu.VMEM((n_tok, HALF_DIM), F32),
            pltpu.VMEM((4, 8, q_len), F32),
            pltpu.VMEM((n_tok, HALF_DIM), F32),
            pltpu.VMEM((n_tok, HALF_DIM), F32),
            pltpu.VMEM((8, 1, dim), F32),
            pltpu.VMEM((q_len, dim), F32),
            pltpu.VMEM((q_len, F_TILE), BF16),
            pltpu.VMEM((2, dim, q_wide + 2 * HEAD_DIM), BF16),
            pltpu.VMEM((2, q_wide, dim), BF16),
            pltpu.VMEM((2, dim, F_TILE), BF16),
            pltpu.VMEM((2, dim, F_TILE), BF16),
            pltpu.VMEM((2, F_TILE, dim), BF16),
            pltpu.SemaphoreType.DMA((2, 4)),
            pltpu.SemaphoreType.DMA((3, 2)),
            pltpu.SemaphoreType.DMA((2, n_chips)),
            pltpu.SemaphoreType.DMA((2, n_chips)),
            pltpu.SemaphoreType.DMA((n_chips, 2)),
            pltpu.SemaphoreType.DMA((cp_size,)),
            pltpu.SemaphoreType.DMA((2, 2, 2)),
            pltpu.SemaphoreType.DMA((2, 2, 2)),
            pltpu.SemaphoreType.DMA((2, n_chips)),
            pltpu.SemaphoreType.DMA((2, n_chips)),
        ]
        return pl.pallas_call(
            functools.partial(fused_kernel, cp_size),
            out_shape=jax.ShapeDtypeStruct(hidden.shape, BF16),
            in_specs=[hbm] + [vmem] * 10 + [hbm] * 14,
            out_specs=hbm,
            scratch_shapes=scratch,
            compiler_params=pltpu.CompilerParams(collective_id=0, has_side_effects=True, vmem_limit_bytes=67043328),
            name="two_layers",
        )(hidden, positions, inv_freq, *scales, *matrices)

    specs_in = tuple([P("dp", "cp"), P("dp", "cp")] + [P()] * 22)
    return jax.shard_map(device_step, mesh=mesh, in_specs=specs_in, out_specs=P("dp", "cp"), check_vma=False)
```

```python
import functools

import jax
import jax.numpy as jnp
import numpy as np
from jax import lax
from jax.experimental import pallas as pl
from jax.experimental.pallas import tpu as pltpu
from jax.sharding import PartitionSpec as P

HEAD_DIM = 256
HALF_DIM = HEAD_DIM // 2
WINDOW = 512
EPSILON = 1e-6
THETA = 10000.0
SOFT_CAP = 50.0
LOG2E = 1.4426950408889634
GELU_A = 0.7978845608028654
F_TILE = 2304
F_SUB = 256
GROUP = 64
BF16 = jnp.bfloat16
F32 = jnp.float32


def dot(lhs, rhs):
    return jnp.dot(lhs, rhs, preferred_element_type=F32)


def gelu_times(gate, up):
    gate = gate.astype(BF16).astype(F32)
    up = up.astype(BF16).astype(F32)
    inner = gate * (GELU_A + (GELU_A * 0.044715) * (gate * gate))
    scaled = (0.5 * gate) * up
    return (scaled + scaled * jnp.tanh(inner)).astype(BF16)


def rms(rows, scale):
    mean_sq = jnp.mean(rows * rows, axis=-1, keepdims=True)
    return (rows * lax.rsqrt(mean_sq + EPSILON) * scale).astype(BF16)


def rope(raw, cos_t, sin_t):
    raw = raw.astype(BF16).astype(F32)
    first, second = raw[:, :HALF_DIM], raw[:, HALF_DIM:]
    return first * cos_t - second * sin_t, second * cos_t + first * sin_t


def fused_kernel(cp_size, hidden, positions, inv_freq, *refs):
    raw_scales = (refs[0:4], refs[4:8])
    weights = (refs[8:15], refs[15:22])
    out = refs[22]
    (xb, ab, mb, qs, kb, vb, ob, mid_b, sum_b, mask_b, ptile, posb, pcol, prow, cos_b, sin_b, scales, acc, hb, w_qkv, w_o, w_g, w_u, w_d,
     w_sem, ring_sem, x_send, x_recv, p_send, p_recv, kv_send, kv_recv, o_send, o_recv) = refs[23:]
    n_chips = cp_size // 2
    piece = hidden.shape[1]
    dim = hidden.shape[2]
    n_tok = xb.shape[1]
    slots = n_tok // piece
    quarter = slots // 2
    q_len = n_tok // 2
    n_heads = w_o.shape[0] // HEAD_DIM
    q_wide = n_heads * HEAD_DIM
    me = lax.axis_index("cp")
    chip, core = me // 2, me % 2
    my_quarter = me // quarter
    my_core = jnp.where((my_quarter == 0) | (my_quarter == 3), 0, 1)
    my_slot = me % quarter + jnp.where(my_quarter >= 2, quarter, 0)

    def quarter_of(which_core, idx):
        return which_core + idx * (3 - 2 * which_core)

    def rows_of(start, size):
        return pl.ds(pl.multiple_of(start, size), size)

    def attention_weights(layer):
        wq, wk, wv, wo = weights[layer][:4]
        return (
            pltpu.make_async_copy(wq, w_qkv.at[:, pl.ds(0, q_wide)], w_sem.at[0]),
            pltpu.make_async_copy(wk, w_qkv.at[:, pl.ds(q_wide, HEAD_DIM)], w_sem.at[1]),
            pltpu.make_async_copy(wv, w_qkv.at[:, pl.ds(q_wide + HEAD_DIM, HEAD_DIM)], w_sem.at[2]),
            pltpu.make_async_copy(wo, w_o, w_sem.at[3]),
        )

    def tile_copies(layer, tile, buf):
        gate, up, down = weights[layer][4:7]
        cols = rows_of(tile * F_TILE, F_TILE)
        return (
            pltpu.make_async_copy(gate.at[:, cols], w_g.at[buf], ring_sem.at[0, buf]),
            pltpu.make_async_copy(up.at[:, cols], w_u.at[buf], ring_sem.at[1, buf]),
            pltpu.make_async_copy(down.at[cols, :], w_d.at[buf], ring_sem.at[2, buf]),
        )

    def start_tile(layer, tile, buf):
        for which in range(2):
            @pl.when(layer == which)
            def _():
                for copy in tile_copies(which, tile, buf):
                    copy.start()

    pos = positions[...].astype(F32)
    pos = jnp.concatenate([pos, pos], axis=1)
    for to_chip in range(n_chips):
        for half in range(2):
            row = half * n_chips + to_chip
            ptile[to_chip, pl.ds(half, 1), :] = pos[row:row + 1, :]
    for layer in range(2):
        for which in range(4):
            scales[layer * 4 + which] = 1.0 + raw_scales[layer][which][...].reshape(1, dim)

    barrier = pltpu.get_barrier_semaphore()
    for shift in range(1, cp_size):
        pl.semaphore_signal(barrier, inc=1, device_id={"cp": lax.rem(me + shift, cp_size)}, device_id_type=pl.DeviceIdType.MESH)
    pl.semaphore_wait(barrier, cp_size - 1)

    def x_copy(half, to_chip):
        return pltpu.make_async_remote_copy(
            src_ref=hidden.at[half * n_chips + to_chip], dst_ref=xb.at[half, rows_of(my_slot * piece, piece), :],
            send_sem=x_send.at[half, to_chip], recv_sem=x_recv.at[half, my_slot],
            device_id={"cp": 2 * to_chip + my_core}, device_id_type=pl.DeviceIdType.MESH)

    def p_copy(to_chip, to_core):
        return pltpu.make_async_remote_copy(
            src_ref=ptile.at[to_chip], dst_ref=posb.at[me], send_sem=p_send.at[to_chip, to_core], recv_sem=p_recv.at[me],
            device_id={"cp": 2 * to_chip + to_core}, device_id_type=pl.DeviceIdType.MESH)

    def each_chip(parity):
        for step in (2, 1, 3, 0):
            yield 2 * lax.rem(chip // 2 + step, n_chips // 2) + parity

    def unless_me(target, copy_call, local_call):
        @pl.when(target != me)
        def _():
            copy_call()

        if local_call is not None:
            @pl.when(target == me)
            def _():
                local_call()

    for parity in range(2):
        for to_chip in each_chip(parity):
            for to_core in range(2):
                unless_me(2 * to_chip + to_core, lambda: p_copy(to_chip, to_core).start(),
                          lambda: pltpu.make_async_copy(ptile.at[to_chip], posb.at[me], p_recv.at[me]).start())
    for half in range(2):
        for parity in range(2):
            for to_chip in each_chip(parity):
                unless_me(2 * to_chip + my_core, lambda: x_copy(half, to_chip).start(),
                          lambda: pltpu.make_async_copy(hidden.at[half * n_chips + to_chip], xb.at[half, rows_of(my_slot * piece, piece), :], x_recv.at[half, my_slot]).start())

    for copy in attention_weights(0):
        copy.start()
    for buf in range(2):
        start_tile(0, buf, buf)
    for from_piece in range(cp_size):
        pltpu.make_async_copy(ptile.at[0], posb.at[from_piece], p_recv.at[from_piece]).wait()
    for copy in attention_weights(0):
        copy.wait()

    def kv_copy(slot, idx, which, owner):
        buf = (kb, vb)[which]
        rows = rows_of(quarter_of(owner, idx) * q_len, q_len)
        return pltpu.make_async_remote_copy(
            src_ref=buf.at[slot, rows, :], dst_ref=buf.at[slot, rows, :], send_sem=kv_send.at[slot, idx, which],
            recv_sem=kv_recv.at[slot, idx, which], device_id={"cp": 2 * chip + 1 - core}, device_id_type=pl.DeviceIdType.MESH)

    def o_target(idx, j):
        return quarter_of(core, idx) * quarter + j

    def o_copy(half, idx, j):
        slot = idx * quarter + j
        return pltpu.make_async_remote_copy(
            src_ref=xb.at[half, rows_of(slot * piece, piece), :], dst_ref=out.at[half * n_chips + chip],
            send_sem=o_send.at[half, slot], recv_sem=o_recv.at[half, chip],
            device_id={"cp": o_target(idx, j)}, device_id_type=pl.DeviceIdType.MESH)

    def take_half(half):
        for slot in range(slots):
            pltpu.make_async_copy(hidden.at[0], xb.at[half, pl.ds(slot * piece, piece), :], x_recv.at[half, slot]).wait()
        lane = lax.broadcasted_iota(jnp.int32, (1, 2 * piece), 1)
        for quad in range(4):
            for pair in range(quarter // 2):
                even = posb[quad * quarter + 2 * pair, pl.ds(half, 1), :]
                odd = posb[quad * quarter + 2 * pair + 1, pl.ds(half, 1), :]
                prow[half, quad, :, pl.ds(pair * 2 * piece, 2 * piece)] = jnp.broadcast_to(jnp.where(lane < piece, even, odd), (8, 2 * piece))
        for idx in range(2):
            for pair in range(quarter // 2):
                line = prow[half, quarter_of(core, idx), pl.ds(0, 1), pl.ds(pair * 2 * piece, 2 * piece)]
                column = jnp.broadcast_to(line, (2 * piece, 2 * piece)).T
                rows = pl.ds(idx * q_len + pair * 2 * piece, 2 * piece)
                pcol[half, rows, :] = column
                angle = column * inv_freq[...]
                cos_b[half, rows, :] = jnp.cos(angle)
                sin_b[half, rows, :] = jnp.sin(angle)

    idx_rows = (pl.ds(0, q_len), pl.ds(q_len, q_len))
    mine = (quarter_of(core, 0), quarter_of(core, 1))
    pairs = ((0, mine[0]), (1, mine[1]), (1, mine[0]), (1 - core, jnp.where(core == 0, 1, 0)), (1, jnp.where(core == 0, 2, 0)))
    to_first = jnp.where(core == 1, 1.0, 0.0)
    to_second = 1.0 - to_first

    def steps_keys(layer, half):
        pre_att = scales[layer * 4]

        def norm_in(group):
            for step in range(group * GROUP, (group + 1) * GROUP, 16):
                rows = pl.ds(step, 16)
                ab[rows, :] = rms(xb[half, rows, :].astype(F32), pre_att)

        def make_keys(idx):
            home = rows_of(mine[idx] * q_len, q_len)
            kv = dot(ab[idx_rows[idx], :], w_qkv[:, q_wide:])
            low, high = rope(kv[:, :HEAD_DIM], cos_b[half, idx_rows[idx], :], sin_b[half, idx_rows[idx], :])
            kb[half, home, pl.ds(0, HALF_DIM)] = low.astype(BF16)
            kb[half, home, pl.ds(HALF_DIM, HALF_DIM)] = high.astype(BF16)
            vb[half, home, :] = kv[:, HEAD_DIM:].astype(BF16)

        def make_mask(number):
            idx, block = pairs[number]
            centre = jnp.where(layer == 0, (WINDOW - 1) * 0.5, n_tok * 2.0 - 0.5)
            here = pcol[half, rows_of(idx * q_len, q_len), :] - centre
            there = prow[half, block, pl.ds(0, 1), :]
            for part in range(2):
                lanes = pl.ds(part * HALF_DIM, HALF_DIM)
                seen = jnp.abs(here - there[:, part * HALF_DIM:(part + 1) * HALF_DIM]) <= centre
                mask_b[number, :, lanes] = jnp.where(seen, 1.0, 0.0)

        groups = n_tok // GROUP
        return ([functools.partial(norm_in, g) for g in range(groups // 2)] + [functools.partial(make_keys, 0)]
                + [functools.partial(norm_in, g) for g in range(groups // 2, groups)] + [functools.partial(make_keys, 1)]
                + [functools.partial(make_mask, number) for number in range(5)])

    def score(half, unit):
        head, number = unit
        idx, block = pairs[number]
        return lax.dot_general(qs[idx, pl.ds(head * q_len, q_len), :], kb[half, rows_of(block * q_len, q_len), :],
                               (((1,), (1,)), ((), ())), preferred_element_type=F32)

    def weigh(half, unit, scores):
        head, number = unit
        idx, block = pairs[number]
        expd = jnp.exp2((SOFT_CAP * LOG2E) * jnp.tanh(scores * (1.0 / SOFT_CAP))) * mask_b[number]
        return expd[:, :HALF_DIM] + expd[:, HALF_DIM:], dot(expd.astype(BF16), vb[half, rows_of(block * q_len, q_len), :])

    def wide(head):
        return pl.ds(head * HEAD_DIM, HEAD_DIM)

    def unit_steps(half, units, before, last):
        state = {"found": []}

        def run(place):
            unit = units[place]
            for call in before.get(place, ()):
                call()
            scores = state["ahead"] if place else score(half, unit)
            if place + 1 < len(units):
                state["ahead"] = score(half, units[place + 1])
            state["found"].append(weigh(half, unit, scores))
            if place + 1 == len(units) or units[place + 1][0] != unit[0]:
                last(unit[0], state["found"])
                state["found"] = []

        return [functools.partial(run, place) for place in range(len(units))]

    def steps_own(layer, half):
        def make_query(head):
            for idx in range(2):
                raw = dot(ab[idx_rows[idx], :], w_qkv[:, wide(head)])
                low, high = rope(raw, cos_b[half, idx_rows[idx], :], sin_b[half, idx_rows[idx], :])
                there = pl.ds(head * q_len, q_len)
                qs[idx, there, pl.ds(0, HALF_DIM)] = (low * HEAD_DIM ** -0.5).astype(BF16)
                qs[idx, there, pl.ds(HALF_DIM, HALF_DIM)] = (high * HEAD_DIM ** -0.5).astype(BF16)

        def last(head, found):
            sum_b[head, idx_rows[0], :] = found[0][0]
            mid_b[idx_rows[0], wide(head)] = found[0][1]
            sum_b[head, idx_rows[1], :] = found[1][0] + found[2][0]
            mid_b[idx_rows[1], wide(head)] = found[1][1] + found[2][1]

        units = [(head, number) for head in range(n_heads) for number in range(3)]
        before = {3 * head: (functools.partial(make_query, head + 1),) for head in range(n_heads - 1)}
        return [functools.partial(make_query, 0)] + unit_steps(half, units, before, last)

    def steps_rest(layer, half):
        post_att, pre_ffw = scales[layer * 4 + 1], scales[layer * 4 + 2]

        def last(head, found):
            totals = (sum_b[head, idx_rows[0], :] + to_first * found[0][0], (sum_b[head, idx_rows[1], :] + found[1][0]) + to_second * found[0][0])
            mixed = (mid_b[idx_rows[0], wide(head)] + to_first * found[0][1], (mid_b[idx_rows[1], wide(head)] + found[1][1]) + to_second * found[0][1])
            for idx in range(2):
                share = 1.0 / jnp.sum(totals[idx], axis=1, keepdims=True)
                ob[idx_rows[idx], wide(head)] = (mixed[idx] * share).astype(BF16)

        def project(idx):
            mid_b[idx_rows[idx], pl.ds(0, dim)] = dot(ob[idx_rows[idx], :], w_o[...])

        def norm_mid(group):
            for step in range(group * GROUP, (group + 1) * GROUP, 16):
                rows = pl.ds(step, 16)
                attn = mid_b[rows, pl.ds(0, dim)].astype(BF16).astype(F32)
                mid = (xb[half, rows, :].astype(F32) + rms(attn, post_att).astype(F32)).astype(BF16)
                xb[half, rows, :] = mid
                ab[rows, :] = rms(mid.astype(F32), pre_ffw)

        units = [(head, number) for head in range(n_heads) for number in (3, 4)]
        groups = n_tok // GROUP
        return (unit_steps(half, units, {}, last) + [functools.partial(project, idx) for idx in range(2)]
                + [functools.partial(norm_mid, g) for g in range(groups)])

    def send_keys(half):
        for idx in range(2):
            for which in range(2):
                kv_copy(half, idx, which, core).start()

    def await_keys(half):
        for idx in range(2):
            for which in range(2):
                kv_copy(half, idx, which, 1 - core).wait_recv()

    def await_sent_keys(half):
        for idx in range(2):
            for which in range(2):
                kv_copy(half, idx, which, core).wait_send()

    late = jnp.where(core == 0, (chip == 3) | (chip >= 5), (chip == 0) | ((chip >= 4) & (chip <= 6))).astype(jnp.int32)

    def part_idx(part):
        return jnp.where(part == 1, late, 1 - late)

    def tile_steps(half, part, buf, start, size, first):
        rows = rows_of(part_idx(part) * q_len + start, size)
        where = pl.ds(0, size)
        there = pl.ds(start, size)

        def up(sub):
            cols = pl.ds(sub * F_SUB, F_SUB)
            hb[where, cols] = gelu_times(dot(mb[rows, :], w_g[buf, :, cols]), dot(mb[rows, :], w_u[buf, :, cols]))

        def down(cols):
            product = dot(hb[where, :], w_d[buf, :, cols])
            acc[part, there, cols] = product if first else acc[part, there, cols] + product

        return ([functools.partial(up, sub) for sub in range(F_TILE // F_SUB)]
                + [functools.partial(down, pl.ds(0, dim // 512 * 256)), functools.partial(down, pl.ds(dim // 512 * 256, dim - dim // 512 * 256))])

    def weave(steps, more):
        done = 0
        for place, step in enumerate(steps):
            step()
            upto = (place + 1) * len(more) // len(steps)
            for other in more[done:upto]:
                other()
            done = upto

    def out_steps(layer, half, part, start, size):
        post_ffw = scales[layer * 4 + 3]

        def norm_out(first_row):
            for step in range(first_row, first_row + min(GROUP, size), 16):
                those = rows_of(part_idx(part) * q_len + step, 16)
                down = acc[part, pl.ds(step, 16), :].astype(BF16).astype(F32)
                xb[half, those, :] = (xb[half, those, :].astype(F32) + rms(down, post_ffw).astype(F32)).astype(BF16)

        return [functools.partial(norm_out, row) for row in range(start, start + size, GROUP)]

    def send_out(half, part, pieces):
        idx = part_idx(part)
        for j in pieces:
            unless_me(o_target(idx, j), lambda: o_copy(half, idx, j).start(),
                      lambda: pltpu.make_async_copy(xb.at[half, rows_of((idx * quarter + j) * piece, piece), :], out.at[half * n_chips + chip], o_recv.at[half, chip]).start())

    def await_tile(buf):
        for copy in tile_copies(0, 0, buf):
            copy.wait()

    def run_all(steps):
        for step in steps:
            step()

    take_half(0)
    run_all(steps_keys(0, 0))
    send_keys(0)
    run_all(steps_own(0, 0))
    await_keys(0)
    run_all(steps_rest(0, 0))
    mb[...] = ab[...]
    await_sent_keys(0)
    last_stage = 3

    def stage(count, carry):
        layer, half = count // 2, count % 2
        after = count + 1
        next_layer, next_half = after // 2, after % 2

        def buf_of(step):
            return (layer + step) % 2

        acc[...] = jnp.zeros_like(acc)

        def plain_tile(number, inner):
            part, step = number // 3, number % 3

            @pl.when((half == 0) | (step == 2))
            def _():
                await_tile(buf_of(step))

            run_all(tile_steps(half, part, buf_of(step), 0, q_len, False))

            @pl.when(step == 0)
            def _():
                start_tile(layer, 2 - 2 * part, buf_of(0))

            @pl.when((count == last_stage) & (step == 2))
            def _():
                run_all(out_steps(layer, half, part, 0, q_len))
                send_out(half, part, range(quarter))

            return inner

        lax.fori_loop(0, jnp.where(count == last_stage, 6, 3), plain_tile, 0)

        @pl.when(count < last_stage)
        def _():
            @pl.when(after < 2)
            def _():
                take_half(next_half)

            @pl.when(after == 2)
            def _():
                for copy in attention_weights(1):
                    copy.wait()

            weave(tile_steps(half, 1, buf_of(0), 0, q_len, True), steps_keys(next_layer, next_half) + out_steps(layer, half, 0, 0, q_len))
            start_tile(layer, 0, buf_of(0))
            send_keys(next_half)

            @pl.when(layer == 1)
            def _():
                send_out(half, 0, range(quarter))

            weave(tile_steps(half, 1, buf_of(1), 0, q_len, False), steps_own(next_layer, next_half))

            @pl.when(count == 1)
            def _():
                start_tile(1, 0, buf_of(1))

            await_keys(next_half)
            await_tile(buf_of(2))
            weave(tile_steps(half, 1, buf_of(2), 0, q_len, False), steps_rest(next_layer, next_half))

            @pl.when(count == 1)
            def _():
                start_tile(1, 1, buf_of(2))

            @pl.when(count == 0)
            def _():
                for copy in attention_weights(1):
                    copy.start()

            run_all(out_steps(layer, half, 1, 0, q_len))
            mb[...] = ab[...]
            await_sent_keys(next_half)

            @pl.when(layer == 1)
            def _():
                send_out(half, 1, range(quarter))

        return carry

    lax.fori_loop(0, 4, stage, 0)

    for half in range(2):
        for idx in range(2):
            for j in range(quarter):
                unless_me(o_target(idx, j), lambda: o_copy(half, idx, j).wait_send(), None)
        for from_chip in range(n_chips):
            pltpu.make_async_copy(xb.at[half, pl.ds(0, piece), :], out.at[half * n_chips + from_chip], o_recv.at[half, from_chip]).wait()
        for to_chip in range(n_chips):
            unless_me(2 * to_chip + my_core, lambda: x_copy(half, to_chip).wait_send(), None)
    for to_chip in range(n_chips):
        for to_core in range(2):
            unless_me(2 * to_chip + to_core, lambda: p_copy(to_chip, to_core).wait_send(), None)


def solution(mesh):
    cp_size = mesh.shape["cp"]

    def device_step(hidden, positions, *weights):
        rows, piece, dim = hidden.shape
        n_chips = cp_size // 2
        n_tok = piece * cp_size // 2
        q_wide = weights[0].shape[1]
        n_heads = q_wide // HEAD_DIM
        q_len = n_tok // 2
        inv_freq = (THETA ** (-(np.arange(HALF_DIM) * 2.0 / HEAD_DIM))).astype(np.float32)[None, :]
        scales = weights[7:11] + weights[18:22]
        matrices = weights[0:7] + weights[11:18]
        hbm = pl.BlockSpec(memory_space=pltpu.HBM)
        vmem = pl.BlockSpec(memory_space=pltpu.VMEM)
        scratch = [
            pltpu.VMEM((2, n_tok, dim), BF16),
            pltpu.VMEM((n_tok, dim), BF16),
            pltpu.VMEM((n_tok, dim), BF16),
            pltpu.VMEM((2, n_heads * q_len, HEAD_DIM), BF16),
            pltpu.VMEM((2, 2 * n_tok, HEAD_DIM), BF16),
            pltpu.VMEM((2, 2 * n_tok, HEAD_DIM), BF16),
            pltpu.VMEM((n_tok, q_wide), BF16),
            pltpu.VMEM((n_tok, max(dim, q_wide)), F32),
            pltpu.VMEM((n_heads, n_tok, HALF_DIM), F32),
            pltpu.VMEM((5, q_len, q_len), F32),
            pltpu.VMEM((n_chips, 8, 2 * piece), F32),
            pltpu.VMEM((cp_size, 8, 2 * piece), F32),
            pltpu.VMEM((2, n_tok, HALF_DIM), F32),
            pltpu.VMEM((2, 4, 8, q_len), F32),
            pltpu.VMEM((2, n_tok, HALF_DIM), F32),
            pltpu.VMEM((2, n_tok, HALF_DIM), F32),
            pltpu.VMEM((8, 1, dim), F32),
            pltpu.VMEM((2, q_len, dim), F32),
            pltpu.VMEM((q_len, F_TILE), BF16),
            pltpu.VMEM((dim, q_wide + 2 * HEAD_DIM), BF16),
            pltpu.VMEM((q_wide, dim), BF16),
            pltpu.VMEM((2, dim, F_TILE), BF16),
            pltpu.VMEM((2, dim, F_TILE), BF16),
            pltpu.VMEM((2, F_TILE, dim), BF16),
            pltpu.SemaphoreType.DMA((4,)),
            pltpu.SemaphoreType.DMA((3, 2)),
            pltpu.SemaphoreType.DMA((2, n_chips)),
            pltpu.SemaphoreType.DMA((2, n_chips)),
            pltpu.SemaphoreType.DMA((n_chips, 2)),
            pltpu.SemaphoreType.DMA((cp_size,)),
            pltpu.SemaphoreType.DMA((2, 2, 2)),
            pltpu.SemaphoreType.DMA((2, 2, 2)),
            pltpu.SemaphoreType.DMA((2, n_chips)),
            pltpu.SemaphoreType.DMA((2, n_chips)),
        ]
        return pl.pallas_call(
            functools.partial(fused_kernel, cp_size),
            out_shape=jax.ShapeDtypeStruct(hidden.shape, BF16),
            in_specs=[hbm] + [vmem] * 10 + [hbm] * 14,
            out_specs=hbm,
            scratch_shapes=scratch,
            compiler_params=pltpu.CompilerParams(collective_id=0, has_side_effects=True, vmem_limit_bytes=67043328),
            name="two_layers",
        )(hidden, positions, inv_freq, *scales, *matrices)

    specs_in = tuple([P("dp", "cp"), P("dp", "cp")] + [P()] * 22)
    return jax.shard_map(device_step, mesh=mesh, in_specs=specs_in, out_specs=P("dp", "cp"), check_vma=False)
```

```python
import functools

import jax
import jax.numpy as jnp
import numpy as np
from jax import lax
from jax.experimental import pallas as pl
from jax.experimental.pallas import tpu as pltpu
from jax.sharding import PartitionSpec as P

HEAD_DIM = 256
HALF_DIM = HEAD_DIM // 2
WINDOW = 512
EPSILON = 1e-6
THETA = 10000.0
SOFT_CAP = 50.0
LOG2E = 1.4426950408889634
GELU_A = 0.7978845608028654
F_TILE = 2304
F_SUB = 256
GROUP = 64
BF16 = jnp.bfloat16
F32 = jnp.float32


def dot(lhs, rhs):
    return jnp.dot(lhs, rhs, preferred_element_type=F32)


def gelu_times(gate, up):
    gate = gate.astype(BF16).astype(F32)
    up = up.astype(BF16).astype(F32)
    inner = gate * (GELU_A + (GELU_A * 0.044715) * (gate * gate))
    scaled = (0.5 * gate) * up
    return (scaled + scaled * jnp.tanh(inner)).astype(BF16)


def rms(rows, scale):
    mean_sq = jnp.mean(rows * rows, axis=-1, keepdims=True)
    return (rows * lax.rsqrt(mean_sq + EPSILON) * scale).astype(BF16)


def rope(raw, cos_t, sin_t):
    raw = raw.astype(BF16).astype(F32)
    first, second = raw[:, :HALF_DIM], raw[:, HALF_DIM:]
    return first * cos_t - second * sin_t, second * cos_t + first * sin_t


def fused_kernel(cp_size, hidden, positions, inv_freq_in, *refs):
    weights = (refs[8:15], refs[15:22])
    out = refs[22]
    (xb, ab, mb, qs, kb, vb, ob, mid_b, sum_b, mask_b, ptile, posb, pcol, prow, cos_b, sin_b, scales, acc, hb, w_qkv, w_o, w_g, w_u, w_d,
     w_sem, ring_sem, x_send, x_recv, p_send, p_recv, kv_send, kv_recv, o_send, o_recv) = refs[23:-11]
    pos_in, inv_freq, small_sem = refs[-11:-8]
    raw_scales = refs[-8:]
    n_chips = cp_size // 2
    piece = hidden.shape[1]
    dim = hidden.shape[2]
    n_tok = xb.shape[1]
    slots = n_tok // piece
    quarter = slots // 2
    q_len = n_tok // 2
    n_heads = w_o.shape[0] // HEAD_DIM
    q_wide = n_heads * HEAD_DIM
    me = lax.axis_index("cp")
    chip, core = me // 2, me % 2
    my_quarter = me // quarter
    my_core = jnp.where((my_quarter == 0) | (my_quarter == 3), 0, 1)
    my_slot = me % quarter + jnp.where(my_quarter >= 2, quarter, 0)

    def quarter_of(which_core, idx):
        return which_core + idx * (3 - 2 * which_core)

    def rows_of(start, size):
        return pl.ds(start if isinstance(start, int) else pl.multiple_of(start, size), size)

    def attention_weights(layer):
        wq, wk, wv, wo = weights[layer][:4]
        return (
            pltpu.make_async_copy(wq, w_qkv.at[:, pl.ds(0, q_wide)], w_sem.at[0]),
            pltpu.make_async_copy(wk, w_qkv.at[:, pl.ds(q_wide, HEAD_DIM)], w_sem.at[1]),
            pltpu.make_async_copy(wv, w_qkv.at[:, pl.ds(q_wide + HEAD_DIM, HEAD_DIM)], w_sem.at[2]),
            pltpu.make_async_copy(wo, w_o, w_sem.at[3]),
        )

    def tile_copies(layer, tile, buf):
        gate, up, down = weights[layer][4:7]
        cols = rows_of(tile * F_TILE, F_TILE)
        return (
            pltpu.make_async_copy(gate.at[:, cols], w_g.at[buf], ring_sem.at[0, buf]),
            pltpu.make_async_copy(up.at[:, cols], w_u.at[buf], ring_sem.at[1, buf]),
            pltpu.make_async_copy(down.at[cols, :], w_d.at[buf], ring_sem.at[2, buf]),
        )

    def start_tile(layer, tile, buf):
        for which in range(2):
            @pl.when(layer == which)
            def _():
                for copy in tile_copies(which, tile, buf):
                    copy.start()

    small = [pltpu.make_async_copy(positions, pos_in, small_sem.at[0]), pltpu.make_async_copy(inv_freq_in, inv_freq, small_sem.at[1])]
    small += [pltpu.make_async_copy(refs[which], raw_scales[which], small_sem.at[2 + which]) for which in range(8)]
    for copy in small:
        copy.start()
    barrier = pltpu.get_barrier_semaphore()
    for shift in range(1, cp_size):
        pl.semaphore_signal(barrier, inc=1, device_id={"cp": lax.rem(me + shift, cp_size)}, device_id_type=pl.DeviceIdType.MESH)
    for copy in attention_weights(0):
        copy.start()
    for buf in range(2):
        start_tile(0, buf, buf)
    small[0].wait()
    pos = pos_in[...].astype(F32)
    pos = jnp.concatenate([pos, pos], axis=1)
    for to_chip in range(n_chips):
        for half in range(2):
            row = half * n_chips + to_chip
            ptile[to_chip, pl.ds(half, 1), :] = pos[row:row + 1, :]
    pl.semaphore_wait(barrier, cp_size - 1)

    def x_copy(half, to_chip):
        return pltpu.make_async_remote_copy(
            src_ref=hidden.at[half * n_chips + to_chip], dst_ref=xb.at[half, rows_of(my_slot * piece, piece), :],
            send_sem=x_send.at[half, to_chip], recv_sem=x_recv.at[half, my_slot],
            device_id={"cp": 2 * to_chip + my_core}, device_id_type=pl.DeviceIdType.MESH)

    def p_copy(to_chip, to_core):
        return pltpu.make_async_remote_copy(
            src_ref=ptile.at[to_chip], dst_ref=posb.at[me], send_sem=p_send.at[to_chip, to_core], recv_sem=p_recv.at[me],
            device_id={"cp": 2 * to_chip + to_core}, device_id_type=pl.DeviceIdType.MESH)

    def each_chip(parity):
        for step in (0, 1, 3, 2):
            yield 2 * lax.rem(chip // 2 + step, n_chips // 2) + parity

    def unless_me(target, copy_call, local_call):
        @pl.when(target != me)
        def _():
            copy_call()

        if local_call is not None:
            @pl.when(target == me)
            def _():
                local_call()

    for parity in range(2):
        for to_chip in each_chip(parity):
            for to_core in range(2):
                unless_me(2 * to_chip + to_core, lambda: p_copy(to_chip, to_core).start(),
                          lambda: pltpu.make_async_copy(ptile.at[to_chip], posb.at[me], p_recv.at[me]).start())
    for half in range(2):
        for parity in range(2):
            for to_chip in each_chip(parity):
                unless_me(2 * to_chip + my_core, lambda: x_copy(half, to_chip).start(),
                          lambda: pltpu.make_async_copy(hidden.at[half * n_chips + to_chip], xb.at[half, rows_of(my_slot * piece, piece), :], x_recv.at[half, my_slot]).start())

    for copy in small[1:]:
        copy.wait()
    for which in range(8):
        scales[which] = 1.0 + raw_scales[which][...].reshape(1, dim)
    for from_piece in range(cp_size):
        pltpu.make_async_copy(ptile.at[0], posb.at[from_piece], p_recv.at[from_piece]).wait()
    for copy in attention_weights(0):
        copy.wait()

    def kv_copy(slot, idx, which, owner):
        buf = (kb, vb)[which]
        rows = rows_of(quarter_of(owner, idx) * q_len, q_len)
        return pltpu.make_async_remote_copy(
            src_ref=buf.at[slot, rows, :], dst_ref=buf.at[slot, rows, :], send_sem=kv_send.at[slot, idx, which],
            recv_sem=kv_recv.at[slot, idx, which], device_id={"cp": 2 * chip + 1 - core}, device_id_type=pl.DeviceIdType.MESH)

    def o_target(idx, j):
        return quarter_of(core, idx) * quarter + j

    def o_copy(half, idx, j):
        slot = idx * quarter + j
        return pltpu.make_async_remote_copy(
            src_ref=xb.at[half, rows_of(slot * piece, piece), :], dst_ref=out.at[half * n_chips + chip],
            send_sem=o_send.at[half, slot], recv_sem=o_recv.at[half, chip],
            device_id={"cp": o_target(idx, j)}, device_id_type=pl.DeviceIdType.MESH)

    def take_half(half):
        for slot in range(slots):
            pltpu.make_async_copy(hidden.at[0], xb.at[half, pl.ds(slot * piece, piece), :], x_recv.at[half, slot]).wait()
        lane = lax.broadcasted_iota(jnp.int32, (1, 2 * piece), 1)
        for quad in range(4):
            for pair in range(quarter // 2):
                even = posb[quad * quarter + 2 * pair, pl.ds(half, 1), :]
                odd = posb[quad * quarter + 2 * pair + 1, pl.ds(half, 1), :]
                prow[half, quad, :, pl.ds(pair * 2 * piece, 2 * piece)] = jnp.broadcast_to(jnp.where(lane < piece, even, odd), (8, 2 * piece))
        for idx in range(2):
            for pair in range(quarter // 2):
                line = prow[half, quarter_of(core, idx), pl.ds(0, 1), pl.ds(pair * 2 * piece, 2 * piece)]
                column = jnp.broadcast_to(line, (2 * piece, 2 * piece)).T
                rows = pl.ds(idx * q_len + pair * 2 * piece, 2 * piece)
                pcol[half, rows, :] = column
                angle = column * inv_freq[...]
                cos_b[half, rows, :] = jnp.cos(angle)
                sin_b[half, rows, :] = jnp.sin(angle)

    idx_rows = (pl.ds(0, q_len), pl.ds(q_len, q_len))
    mine = (quarter_of(core, 0), quarter_of(core, 1))
    pairs = ((0, mine[0]), (1, mine[1]), (1, mine[0]), (1 - core, jnp.where(core == 0, 1, 0)), (1, jnp.where(core == 0, 2, 0)))
    to_first = jnp.where(core == 1, 1.0, 0.0)
    to_second = 1.0 - to_first

    def steps_keys(layer, half):
        pre_att = scales[layer * 4]

        def norm_in(group):
            for step in range(group * GROUP, (group + 1) * GROUP, 16):
                rows = pl.ds(step, 16)
                ab[rows, :] = rms(xb[half, rows, :].astype(F32), pre_att)

        def make_keys(idx):
            home = rows_of(mine[idx] * q_len, q_len)
            kv = dot(ab[idx_rows[idx], :], w_qkv[:, q_wide:])
            low, high = rope(kv[:, :HEAD_DIM], cos_b[half, idx_rows[idx], :], sin_b[half, idx_rows[idx], :])
            kb[half, home, pl.ds(0, HALF_DIM)] = low.astype(BF16)
            kb[half, home, pl.ds(HALF_DIM, HALF_DIM)] = high.astype(BF16)
            vb[half, home, :] = kv[:, HEAD_DIM:].astype(BF16)

        def make_mask(number):
            idx, block = pairs[number]
            centre = jnp.where(layer == 0, (WINDOW - 1) * 0.5, n_tok * 2.0 - 0.5)
            here = pcol[half, rows_of(idx * q_len, q_len), :] - centre
            there = prow[half, block, pl.ds(0, 1), :]
            for part in range(2):
                lanes = pl.ds(part * HALF_DIM, HALF_DIM)
                seen = jnp.abs(here - there[:, part * HALF_DIM:(part + 1) * HALF_DIM]) <= centre
                mask_b[number, :, lanes] = jnp.where(seen, 1.0, 0.0)

        groups = n_tok // GROUP
        return ([functools.partial(norm_in, g) for g in range(groups // 2)] + [functools.partial(make_keys, 0)]
                + [functools.partial(norm_in, g) for g in range(groups // 2, groups)] + [functools.partial(make_keys, 1)]
                + [functools.partial(make_mask, number) for number in range(5)])

    def score(half, unit):
        head, number = unit
        idx, block = pairs[number]
        return lax.dot_general(qs[idx, rows_of(head * q_len, q_len), :], kb[half, rows_of(block * q_len, q_len), :],
                               (((1,), (1,)), ((), ())), preferred_element_type=F32)

    def weigh(half, unit, scores):
        head, number = unit
        idx, block = pairs[number]
        expd = jnp.exp2((SOFT_CAP * LOG2E) * jnp.tanh(scores * (1.0 / SOFT_CAP))) * mask_b[number]
        return expd[:, :HALF_DIM] + expd[:, HALF_DIM:], dot(expd.astype(BF16), vb[half, rows_of(block * q_len, q_len), :])

    def wide(head):
        return rows_of(head * HEAD_DIM, HEAD_DIM)

    def unit_steps(half, units, before, last):
        state = {"found": []}

        def run(place):
            unit = units[place]
            for call in before.get(place, ()):
                call()
            scores = state["ahead"] if place else score(half, unit)
            if place + 1 < len(units):
                state["ahead"] = score(half, units[place + 1])
            state["found"].append(weigh(half, unit, scores))
            if place + 1 == len(units) or units[place + 1][0] is not unit[0]:
                last(unit[0], state["found"])
                state["found"] = []

        return [functools.partial(run, place) for place in range(len(units))]

    def steps_own(layer, half, only=None):
        def make_query(head):
            for idx in range(2):
                raw = dot(ab[idx_rows[idx], :], w_qkv[:, wide(head)])
                low, high = rope(raw, cos_b[half, idx_rows[idx], :], sin_b[half, idx_rows[idx], :])
                there = rows_of(head * q_len, q_len)
                qs[idx, there, pl.ds(0, HALF_DIM)] = (low * HEAD_DIM ** -0.5).astype(BF16)
                qs[idx, there, pl.ds(HALF_DIM, HALF_DIM)] = (high * HEAD_DIM ** -0.5).astype(BF16)

        def last(head, found):
            sum_b[head, idx_rows[0], :] = found[0][0]
            mid_b[idx_rows[0], wide(head)] = found[0][1]
            sum_b[head, idx_rows[1], :] = found[1][0] + found[2][0]
            mid_b[idx_rows[1], wide(head)] = found[1][1] + found[2][1]

        if only is not None:
            return [functools.partial(make_query, only)] + unit_steps(half, [(only, number) for number in range(3)], {}, last)
        units = [(head, number) for head in range(n_heads) for number in range(3)]
        before = {3 * head: (functools.partial(make_query, head + 1),) for head in range(n_heads - 1)}
        return [functools.partial(make_query, 0)] + unit_steps(half, units, before, last)

    def steps_rest(layer, half, only=None, heads=True):
        post_att, pre_ffw = scales[layer * 4 + 1], scales[layer * 4 + 2]

        def last(head, found):
            totals = (sum_b[head, idx_rows[0], :] + to_first * found[0][0], (sum_b[head, idx_rows[1], :] + found[1][0]) + to_second * found[0][0])
            mixed = (mid_b[idx_rows[0], wide(head)] + to_first * found[0][1], (mid_b[idx_rows[1], wide(head)] + found[1][1]) + to_second * found[0][1])
            for idx in range(2):
                share = 1.0 / jnp.sum(totals[idx], axis=1, keepdims=True)
                ob[idx_rows[idx], wide(head)] = (mixed[idx] * share).astype(BF16)

        def project(idx):
            mid_b[idx_rows[idx], pl.ds(0, dim)] = dot(ob[idx_rows[idx], :], w_o[...])

        def norm_mid(group):
            for step in range(group * GROUP, (group + 1) * GROUP, 16):
                rows = pl.ds(step, 16)
                attn = mid_b[rows, pl.ds(0, dim)].astype(BF16).astype(F32)
                mid = (xb[half, rows, :].astype(F32) + rms(attn, post_att).astype(F32)).astype(BF16)
                xb[half, rows, :] = mid
                ab[rows, :] = rms(mid.astype(F32), pre_ffw)

        units = [(head, number) for head in range(n_heads) for number in (3, 4)]
        groups = n_tok // GROUP
        if only is not None:
            return unit_steps(half, [(only, 3), (only, 4)], {}, last)
        if not heads:
            units = []
        return (unit_steps(half, units, {}, last) + [functools.partial(project, idx) for idx in range(2)]
                + [functools.partial(norm_mid, g) for g in range(groups)])

    def send_keys(half):
        for idx in range(2):
            for which in range(2):
                kv_copy(half, idx, which, core).start()

    def await_keys(half):
        for idx in range(2):
            for which in range(2):
                kv_copy(half, idx, which, 1 - core).wait_recv()

    def await_sent_keys(half):
        for idx in range(2):
            for which in range(2):
                kv_copy(half, idx, which, core).wait_send()

    late = jnp.where(core == 0, (chip == 0) | ((chip >= 4) & (chip <= 6)), (chip == 3) | (chip >= 5)).astype(jnp.int32)

    def part_idx(part):
        return jnp.where(part == 1, late, 1 - late)

    def tile_steps(half, part, buf, start, size, first, only=None):
        rows = rows_of(part_idx(part) * q_len + start, size)
        where = pl.ds(0, size)
        there = rows_of(start, size)

        def up(sub):
            cols = rows_of(sub * F_SUB, F_SUB)
            hb[where, cols] = gelu_times(dot(mb[rows, :], w_g[buf, :, cols]), dot(mb[rows, :], w_u[buf, :, cols]))

        def down(cols):
            product = dot(hb[where, :], w_d[buf, :, cols])
            acc[part, there, cols] = product if first else acc[part, there, cols] + product

        if only is not None:
            return [functools.partial(up, only)]
        return ([functools.partial(up, sub) for sub in range(F_TILE // F_SUB)]
                + [functools.partial(down, pl.ds(0, dim // 512 * 256)), functools.partial(down, pl.ds(dim // 512 * 256, dim - dim // 512 * 256))])

    def weave(steps, more):
        done = 0
        for place, step in enumerate(steps):
            step()
            upto = (place + 1) * len(more) // len(steps)
            for other in more[done:upto]:
                other()
            done = upto

    def out_steps(layer, half, part, start, size):
        post_ffw = scales[layer * 4 + 3]

        def norm_out(first_row):
            for offset in range(0, GROUP, 16):
                step = first_row + offset
                those = rows_of(part_idx(part) * q_len + step, 16)
                down = acc[part, rows_of(step, 16), :].astype(BF16).astype(F32)
                xb[half, those, :] = (xb[half, those, :].astype(F32) + rms(down, post_ffw).astype(F32)).astype(BF16)

        return [functools.partial(norm_out, start + row) for row in range(0, size, GROUP)]

    def send_out(half, part, pieces):
        idx = part_idx(part)
        for j in pieces:
            unless_me(o_target(idx, j), lambda: o_copy(half, idx, j).start(),
                      lambda: pltpu.make_async_copy(xb.at[half, rows_of((idx * quarter + j) * piece, piece), :], out.at[half * n_chips + chip], o_recv.at[half, chip]).start())

    def await_tile(buf):
        for copy in tile_copies(0, 0, buf):
            copy.wait()

    def run_all(steps):
        for step in steps:
            step()

    take_half(0)
    run_all(steps_keys(0, 0))
    send_keys(0)
    run_all(steps_own(0, 0))
    await_keys(0)
    lax.fori_loop(0, n_heads, lambda head, inner: (run_all(steps_rest(0, 0, head)), inner)[1], 0)
    run_all(steps_rest(0, 0, heads=False))
    mb[...] = ab[...]
    await_sent_keys(0)
    last_stage = 3

    def stage(count, carry):
        layer, half = count // 2, count % 2
        after = count + 1
        next_layer, next_half = after // 2, after % 2

        def buf_of(step):
            return (layer + step) % 2

        acc[...] = jnp.zeros_like(acc)

        def plain_tile(number, inner):
            part, step = number // 3, number % 3

            @pl.when((half == 0) | (step == 2))
            def _():
                await_tile(buf_of(step))

            run_all(tile_steps(half, part, buf_of(step), 0, q_len, False))

            @pl.when(step == 0)
            def _():
                start_tile(layer, 2 - 2 * part, buf_of(0))

            @pl.when((count == last_stage) & (step == 2))
            def _():
                run_all(out_steps(layer, half, part, 0, q_len))
                send_out(half, part, range(quarter))

            return inner

        lax.fori_loop(0, jnp.where(count == last_stage, 5, 3), plain_tile, 0)

        @pl.when(count == last_stage)
        def _():
            await_tile(buf_of(2))
            ahead_of_me = lax.rem(2 * quarter_of(core, late) - chip + n_chips, n_chips)
            last_half = jnp.where(ahead_of_me >= n_chips // 2, 1, 0)

            def last_rows(turn, inner):
                piece_half = jnp.where(turn == 1, last_half, 1 - last_half)
                start = piece_half * (q_len // 2)

                def up_steps(third, inner2):
                    for sub in range(3):
                        tile_steps(half, 1, buf_of(2), start, q_len // 2, False, third * 3 + sub)[0]()
                    return inner2

                lax.fori_loop(0, F_TILE // F_SUB // 3, up_steps, 0)
                run_all(tile_steps(half, 1, buf_of(2), start, q_len // 2, False)[-2:])
                run_all(out_steps(layer, half, 1, start, q_len // 2))
                send_out(half, 1, [piece_half * (quarter // 2) + j for j in range(quarter // 2)])
                return inner

            lax.fori_loop(0, 2, last_rows, 0)


        @pl.when(count < last_stage)
        def _():
            @pl.when(after < 2)
            def _():
                take_half(next_half)

            @pl.when(after == 2)
            def _():
                for copy in attention_weights(1):
                    copy.wait()

            weave(tile_steps(half, 1, buf_of(0), 0, q_len, True), steps_keys(next_layer, next_half) + out_steps(layer, half, 0, 0, q_len))
            start_tile(layer, 0, buf_of(0))
            send_keys(next_half)

            @pl.when(layer == 1)
            def _():
                send_out(half, 0, range(quarter))

            weave(tile_steps(half, 1, buf_of(1), 0, q_len, False), steps_own(next_layer, next_half))

            @pl.when(count == 1)
            def _():
                start_tile(1, 0, buf_of(1))

            await_keys(next_half)
            await_tile(buf_of(2))
            weave(tile_steps(half, 1, buf_of(2), 0, q_len, False), steps_rest(next_layer, next_half))

            @pl.when(count == 1)
            def _():
                start_tile(1, 1, buf_of(2))

            @pl.when(count == 0)
            def _():
                for copy in attention_weights(1):
                    copy.start()

            run_all(out_steps(layer, half, 1, 0, q_len))
            mb[...] = ab[...]
            await_sent_keys(next_half)

            @pl.when(layer == 1)
            def _():
                send_out(half, 1, range(quarter))

        return carry

    lax.fori_loop(0, 4, stage, 0)

    for half in range(2):
        for idx in range(2):
            for j in range(quarter):
                unless_me(o_target(idx, j), lambda: o_copy(half, idx, j).wait_send(), None)
        for from_chip in range(n_chips):
            pltpu.make_async_copy(xb.at[half, pl.ds(0, piece), :], out.at[half * n_chips + from_chip], o_recv.at[half, from_chip]).wait()
        for to_chip in range(n_chips):
            unless_me(2 * to_chip + my_core, lambda: x_copy(half, to_chip).wait_send(), None)
    for to_chip in range(n_chips):
        for to_core in range(2):
            unless_me(2 * to_chip + to_core, lambda: p_copy(to_chip, to_core).wait_send(), None)


def solution(mesh):
    cp_size = mesh.shape["cp"]

    def device_step(hidden, positions, *weights):
        rows, piece, dim = hidden.shape
        n_chips = cp_size // 2
        n_tok = piece * cp_size // 2
        q_wide = weights[0].shape[1]
        n_heads = q_wide // HEAD_DIM
        q_len = n_tok // 2
        inv_freq = (THETA ** (-(np.arange(HALF_DIM) * 2.0 / HEAD_DIM))).astype(np.float32)[None, :]
        scales = weights[7:11] + weights[18:22]
        matrices = weights[0:7] + weights[11:18]
        hbm = pl.BlockSpec(memory_space=pltpu.HBM)
        scratch = [
            pltpu.VMEM((2, n_tok, dim), BF16),
            pltpu.VMEM((n_tok, dim), BF16),
            pltpu.VMEM((n_tok, dim), BF16),
            pltpu.VMEM((2, n_heads * q_len, HEAD_DIM), BF16),
            pltpu.VMEM((2, 2 * n_tok, HEAD_DIM), BF16),
            pltpu.VMEM((2, 2 * n_tok, HEAD_DIM), BF16),
            pltpu.VMEM((n_tok, q_wide), BF16),
            pltpu.VMEM((n_tok, max(dim, q_wide)), F32),
            pltpu.VMEM((n_heads, n_tok, HALF_DIM), F32),
            pltpu.VMEM((5, q_len, q_len), F32),
            pltpu.VMEM((n_chips, 8, 2 * piece), F32),
            pltpu.VMEM((cp_size, 8, 2 * piece), F32),
            pltpu.VMEM((2, n_tok, HALF_DIM), F32),
            pltpu.VMEM((2, 4, 8, q_len), F32),
            pltpu.VMEM((2, n_tok, HALF_DIM), F32),
            pltpu.VMEM((2, n_tok, HALF_DIM), F32),
            pltpu.VMEM((8, 1, dim), F32),
            pltpu.VMEM((2, q_len, dim), F32),
            pltpu.VMEM((q_len, F_TILE), BF16),
            pltpu.VMEM((dim, q_wide + 2 * HEAD_DIM), BF16),
            pltpu.VMEM((q_wide, dim), BF16),
            pltpu.VMEM((2, dim, F_TILE), BF16),
            pltpu.VMEM((2, dim, F_TILE), BF16),
            pltpu.VMEM((2, F_TILE, dim), BF16),
            pltpu.SemaphoreType.DMA((4,)),
            pltpu.SemaphoreType.DMA((3, 2)),
            pltpu.SemaphoreType.DMA((2, n_chips)),
            pltpu.SemaphoreType.DMA((2, n_chips)),
            pltpu.SemaphoreType.DMA((n_chips, 2)),
            pltpu.SemaphoreType.DMA((cp_size,)),
            pltpu.SemaphoreType.DMA((2, 2, 2)),
            pltpu.SemaphoreType.DMA((2, 2, 2)),
            pltpu.SemaphoreType.DMA((2, n_chips)),
            pltpu.SemaphoreType.DMA((2, n_chips)),
            pltpu.VMEM(positions.shape, jnp.int32),
            pltpu.VMEM((1, HALF_DIM), F32),
            pltpu.SemaphoreType.DMA((10,)),
        ] + [pltpu.VMEM((dim,), F32)] * 8
        return pl.pallas_call(
            functools.partial(fused_kernel, cp_size),
            out_shape=jax.ShapeDtypeStruct(hidden.shape, BF16),
            in_specs=[hbm] * 25,
            out_specs=hbm,
            scratch_shapes=scratch,
            compiler_params=pltpu.CompilerParams(collective_id=0, has_side_effects=True, vmem_limit_bytes=67043328),
            name="two_layers",
        )(hidden, positions, inv_freq, *scales, *matrices)

    specs_in = tuple([P("dp", "cp"), P("dp", "cp")] + [P()] * 22)
    return jax.shard_map(device_step, mesh=mesh, in_specs=specs_in, out_specs=P("dp", "cp"), check_vma=False)
```
